16 devices in a mesh: dp: 2 (over y, z), tp: 8 (over x, core).
Axes of the slice: x: 4, y: 2, z: 1, core: 2. Of those that a mesh axis runs over, the one named last changes fastest.
The devices are a block of a 4x4x8 slice.
Arguments:
- hidden: bfloat16 [512, 5, 12288], P('dp'), parts along dimension 0
- w_head: bfloat16 [12288, 32768], P(None, 'tp')
- q_draft: float32 [512, 4, 32768], P(('dp', 'tp')), parts along dimension 0
- x_draft: int32 [512, 4], P('dp'), parts along dimension 0
Outputs:
- output 1: float32 [512, 4], P(('dp', 'tp')), parts along dimension 0
- output 2: float32 [512], P(('dp', 'tp')), parts along dimension 0
- output 3: float32 [512, 4, 32768], P(('dp', 'tp')), parts along dimension 0
- output 4: float32 [512, 32768], P(('dp', 'tp')), parts along dimension 0
There are 2 independent parts. The reference program is written for one: setup_inputs(seed, part) draws one part's arguments, and reference() takes and returns one part's arrays. A program takes and returns all parts, laid end to end along the dimension named above; an argument that names none is the same for every part.
All inputs are finite; a program needn't handle non-finite values.
Results may differ from the reference program's by a relative error of at most 0.001.
Values are sent between devices in bfloat16 or wider.
A program may use at most 768 MiB of HBM per device.

```python
import jax
import jax.numpy as jnp
from jax import lax

BATCH = 256
DRAFT = 4
HIDDEN = 12288
VOCAB = 32768
INV_TEMP = 1.25


def draw_tokens(token_key):
    tokens = jax.random.randint(token_key, (BATCH, DRAFT), 0, VOCAB, dtype=jnp.int32)
    return tokens.at[0, 0].set(VOCAB - 1).at[0, 1].set(0)


def setup_inputs(seed: int = 0, part: int = 0) -> dict:
    root_key = jax.random.key(seed)
    shared_key, part_root = jax.random.split(root_key)
    part_key = jax.random.fold_in(part_root, part)
    key_hidden, key_draft, key_token = jax.random.split(part_key, 3)
    raw_hidden = jax.random.normal(key_hidden, (BATCH, DRAFT + 1, HIDDEN), jnp.float32)
    hidden = raw_hidden * lax.rsqrt(jnp.mean(raw_hidden * raw_hidden, axis=-1, keepdims=True) + 1e-6)
    w_head = jax.random.normal(shared_key, (HIDDEN, VOCAB), jnp.float32) * HIDDEN ** -0.5
    draft_logits = 1.25 * jax.random.normal(key_draft, (BATCH, DRAFT, VOCAB), jnp.float32)
    q_draft = jax.nn.softmax(draft_logits, axis=-1)
    return {"hidden": hidden.astype(jnp.bfloat16), "w_head": w_head.astype(jnp.bfloat16), "q_draft": q_draft, "x_draft": draw_tokens(key_token)}


def reference(hidden, w_head, q_draft, x_draft):
    def verify_one(seq_args):
        hidden_seq, q_seq, x_seq = seq_args
        logits = jnp.dot(hidden_seq, w_head, preferred_element_type=jnp.float32) * INV_TEMP
        row_peak = jnp.max(logits, axis=-1, keepdims=True)
        exp_vals = jnp.exp(logits - row_peak)
        target_p = exp_vals / jnp.sum(exp_vals, axis=-1, keepdims=True)
        draft_p = target_p[:DRAFT]
        p_pick = jnp.take_along_axis(draft_p, x_seq[:, None], axis=1)[:, 0]
        q_pick = jnp.take_along_axis(q_seq, x_seq[:, None], axis=1)[:, 0]
        seq_accept = jnp.minimum(1.0, p_pick / q_pick)
        seq_expected = jnp.sum(jnp.cumprod(seq_accept))
        excess = jnp.maximum(draft_p - q_seq, 0.0)
        seq_resid = excess / jnp.sum(excess, axis=-1, keepdims=True)
        return seq_accept, seq_expected, seq_resid, target_p[DRAFT]

    accept, expected, residual, bonus = lax.map(verify_one, (hidden, q_draft, x_draft))
    return accept, expected, residual, bonus
```

```python
import functools

import jax
import jax.numpy as jnp
from jax import lax
from jax.experimental import pallas as pl
from jax.experimental.pallas import tpu as pltpu
from jax.sharding import PartitionSpec as P

INV_TEMP = 1.25
LANES = 128
TILE = 256
DEPTH = 2048
SLOTS = 4
CORES = 2


def exchange_kernel(draft, n_dev, h_ref, w_ref, zd_ref, zb_ref, st_ref, hbuf, wbuf, acc, stgd, stgb, mrun, srun, stst,
                    hsem, wsem, ssd, ssb, sss, lsd, lsb, lss, rsd, rsb, rss):
    npos = draft + 1
    chips = n_dev // CORES
    seq_chip = h_ref.shape[1] // chips
    seq_dev = seq_chip // CORES
    depth_steps = h_ref.shape[2] // DEPTH
    tiles = w_ref.shape[1] // TILE
    lane_blocks = TILE // LANES
    rows_tile = lane_blocks * draft
    me = lax.axis_index("tp")
    chip, core = me // CORES, lax.rem(me, CORES)
    sib = 1 - core

    order = (1, chips - 1, *range(2, chips - 1), 0)

    def chip_at(ci):
        step = order[ci] if isinstance(ci, int) else ci
        return lax.rem(chip + step, chips)

    def h_copy(ci, k):
        c = chip_at(ci)
        view = (slice(None), pl.ds(pl.multiple_of(c * seq_chip, seq_chip), seq_chip), pl.ds(pl.multiple_of(k * DEPTH, DEPTH), DEPTH))
        return pltpu.make_async_copy(h_ref.at[view], hbuf.at[view], hsem.at[ci, k])

    def w_copy(j, k):
        slot = lax.rem(j, 2)
        rows = pl.ds(pl.multiple_of(k * DEPTH, DEPTH), DEPTH)
        return pltpu.make_async_copy(w_ref.at[rows, pl.ds(pl.multiple_of(j * TILE, TILE), TILE)], wbuf.at[slot, rows], wsem.at[slot, k])

    def part(co):
        return tuple(pl.ds(pl.multiple_of(co * n, n), n) for n in (seq_dev * rows_tile, seq_dev))

    def pieces(j, ci):
        slot = lax.rem(j, SLOTS)
        block = me * tiles + j
        cols = pl.ds(pl.multiple_of(me * tiles * TILE + j * TILE, TILE), TILE)
        out = []
        if order[ci] == 0:
            drows, brows = part(core)
            out.append(pltpu.make_async_copy(stgd.at[slot, ci, drows], zd_ref.at[block], lsd.at[slot]))
            out.append(pltpu.make_async_copy(stgb.at[slot, ci, brows], zb_ref.at[:, cols], lsb.at[slot]))
            cores = (sib,)
        else:
            cores = tuple(range(CORES))
        for n, co in enumerate(cores):
            drows, brows = part(co)
            to = {"tp": chip_at(ci) * CORES + co}
            out.append(pltpu.make_async_remote_copy(stgd.at[slot, ci, drows], zd_ref.at[block], ssd.at[slot, ci, n], rsd.at[me], device_id=to))
            out.append(pltpu.make_async_remote_copy(stgb.at[slot, ci, brows], zb_ref.at[:, cols], ssb.at[slot, ci, n], rsb.at[me], device_id=to))
        return out

    def stat_pieces(ci):
        if order[ci] == 0:
            out = [pltpu.make_async_copy(stst.at[ci, core], st_ref.at[me], lss)]
            cores = (sib,)
        else:
            out = []
            cores = tuple(range(CORES))
        for n, co in enumerate(cores):
            to = {"tp": chip_at(ci) * CORES + co}
            out.append(pltpu.make_async_remote_copy(stst.at[ci, co], st_ref.at[me], sss.at[ci, n], rss.at[me], device_id=to))
        return out

    def wait_sent(copies):
        for copy in copies:
            copy.wait_send() if copy.is_remote else copy.wait()

    for k in range(depth_steps):
        h_copy(0, k).start()
        w_copy(0, k).start()

    barrier = pltpu.get_barrier_semaphore()
    for o in range(1, n_dev):
        pl.semaphore_signal(barrier, 1, device_id={"tp": lax.rem(me + o, n_dev)})
    pl.semaphore_wait(barrier, n_dev - 1)

    mrun[...] = jnp.full(mrun.shape, -jnp.inf, jnp.float32)
    srun[...] = jnp.zeros(srun.shape, jnp.float32)

    @pl.loop(0, tiles)
    def _(j):
        wslot = lax.rem(j, 2)
        slot = lax.rem(j, SLOTS)
        for ci in range(chips):
            start = pl.multiple_of(chip_at(ci) * seq_chip, seq_chip)

            @pl.loop(0, depth_steps)
            def _(k):
                @pl.when(j == 0)
                def _():
                    h_copy(ci, k).wait()
                    if ci + 1 < chips:
                        h_copy(ci + 1, k).start()

                if ci == 0:
                    w_copy(j, k).wait()
                if ci == chips // 2:
                    @pl.when(j + 1 < tiles)
                    def _():
                        w_copy(j + 1, k).start()

                cols = pl.ds(pl.multiple_of(k * DEPTH, DEPTH), DEPTH)
                lhs = hbuf[:, pl.ds(start, seq_chip), cols].reshape(npos * seq_chip, DEPTH)
                prod = jnp.dot(lhs, wbuf[wslot, cols, :], preferred_element_type=jnp.float32)

                @pl.when(k == 0)
                def _():
                    acc[...] = prod

                @pl.when(k > 0)
                def _():
                    acc[...] += prod

            @pl.when(j >= SLOTS)
            def _():
                wait_sent(pieces(j - SLOTS, ci))

            for i in range(npos):
                zs = [acc[i * seq_chip:(i + 1) * seq_chip, cc * LANES:(cc + 1) * LANES] * INV_TEMP for cc in range(lane_blocks)]
                m_old = mrun[ci, i]
                m_new = functools.reduce(jnp.maximum, zs, m_old)
                total = srun[ci, i] * jnp.exp(m_old - m_new)
                for cc, z in enumerate(zs):
                    total += jnp.exp(z - m_new)
                    if i < draft:
                        stgd[slot, ci, pl.ds(cc * draft + i, seq_chip, stride=rows_tile), :] = z
                    else:
                        stgb[slot, ci, :, cc * LANES:(cc + 1) * LANES] = z
                mrun[ci, i] = m_new
                srun[ci, i] = total
            for copy in pieces(j, ci):
                copy.start()

    lane = lax.broadcasted_iota(jnp.int32, (seq_chip, LANES), 1)
    for ci in range(chips):
        packed = jnp.zeros((seq_chip, LANES), jnp.float32)
        for i in range(npos):
            m_lane = mrun[ci, i]
            m = jnp.max(m_lane, axis=1, keepdims=True)
            s = jnp.sum(srun[ci, i] * jnp.exp(m_lane - m), axis=1, keepdims=True)
            packed = jnp.where(lane == i, m, packed)
            packed = jnp.where(lane == 8 + i, s, packed)
        flat = jnp.concatenate([packed, jnp.zeros((LANES - seq_chip, LANES), jnp.float32)], axis=0).T[:16]
        for co in range(CORES):
            stst[ci, co] = flat if co == 0 else pltpu.roll(flat, LANES - co * seq_dev, 1)
        for copy in stat_pieces(ci):
            copy.start()

    for j in range(max(0, tiles - SLOTS), tiles):
        for ci in range(chips):
            wait_sent(pieces(j, ci))
    for ci in range(chips):
        wait_sent(stat_pieces(ci))
    for o in range(1, n_dev):
        src = lax.rem(me + o, n_dev)
        zrows = zd_ref.at[pl.ds(src * tiles, tiles)]
        zcols = zb_ref.at[:, pl.ds(pl.multiple_of(src * tiles * TILE, TILE), tiles * TILE)]
        pltpu.make_async_copy(zrows, zrows, rsd.at[src]).wait()
        pltpu.make_async_copy(zcols, zcols, rsb.at[src]).wait()
        pltpu.make_async_copy(st_ref.at[src], st_ref.at[src], rss.at[src]).wait()


def verify_kernel(draft, x_ref, st_ref, zd_ref, zb_ref, q_ref, acc_ref, exp_ref, res_ref, bon_ref, mrow, irow, mcol, icol):
    step = pl.program_id(0)
    per_step = q_ref.shape[0]
    seq_dev = zb_ref.shape[0]
    first = lax.axis_index("tp") * seq_dev + step * per_step
    lane8 = lax.broadcasted_iota(jnp.int32, (8, LANES), 1)

    @pl.when(step == 0)
    def _():
        m_all = st_ref[:, 0:8, :]
        m = jnp.max(m_all, axis=0)
        s = jnp.sum(st_ref[:, 8:16, :] * jnp.exp(m_all - m[None]), axis=0)
        inv = 1.0 / s
        mrow[...] = jnp.concatenate([m[:draft], m[:draft]], axis=0)
        irow[...] = jnp.concatenate([inv[:draft], inv[:draft]], axis=0)
        pad = jnp.zeros((LANES - 8, LANES), jnp.float32)
        mcol[...] = jnp.broadcast_to(jnp.concatenate([m, pad], axis=0).T[:seq_dev, draft:draft + 1], mcol.shape)
        icol[...] = jnp.broadcast_to(jnp.concatenate([inv, pad], axis=0).T[:seq_dev, draft:draft + 1], icol.shape)
        acc_ref[...] = jnp.zeros(acc_ref.shape, jnp.float32)

    tiles = zd_ref.shape[0]
    group = 8
    seqs = range(per_step)

    def column(ref, bb):
        hit = lane8 == step * per_step + bb
        return jnp.broadcast_to(jnp.sum(jnp.where(hit, ref[...], 0.0), axis=1, keepdims=True), (8, LANES))

    m8 = [column(mrow, bb) for bb in seqs]
    i8 = [column(irow, bb) for bb in seqs]

    def sweep(n, totals):
        out = []
        for bb in seqs:
            total = totals[bb]
            for g in range(group):
                z = zd_ref[n * group + g, bb * 8:(bb + 1) * 8, :]
                at = pl.ds(pl.multiple_of((n * group + g) * 8, 8), 8)
                excess = jnp.maximum(jnp.exp(z - m8[bb]) * i8[bb] - q_ref[bb, at, :], 0.0)
                res_ref[bb, at, :] = excess
                total += excess
            out.append(total)
        return tuple(out)

    totals = lax.fori_loop(0, tiles // group, sweep, tuple(jnp.zeros((8, LANES), jnp.float32) for _ in seqs))
    scales = []
    for total in totals:
        total += pltpu.roll(total, draft, 0)
        scales.append(jnp.broadcast_to(1.0 / jnp.sum(total, axis=1, keepdims=True), (8, LANES)))

    def scale(n, carry):
        for bb in seqs:
            for g in range(group):
                at = pl.ds(pl.multiple_of((n * group + g) * 8, 8), 8)
                res_ref[bb, at, :] = res_ref[bb, at, :] * scales[bb]
        return carry

    lax.fori_loop(0, tiles // group, scale, 0)

    lane1 = lax.broadcasted_iota(jnp.int32, (1, LANES), 1)
    lane_b = lax.broadcasted_iota(jnp.int32, acc_ref.shape, 1)
    picked = acc_ref[...]
    for bb in seqs:
        zs, qs = [], []
        for i in range(draft):
            x = x_ref[i, first + bb]
            pair, half = lax.shift_right_logical(x, 8), lax.shift_right_logical(x, 7) & 1
            row = half * draft + i
            hit = lane1 == (x & (LANES - 1))
            zs.append(jnp.where(hit, zd_ref[pair, pl.ds(bb * 8 + row, 1), :], 0.0))
            qs.append(jnp.where(hit, q_ref[bb, pl.ds(pair * 8 + row, 1), :], 0.0))
        z_pick = jnp.sum(jnp.concatenate(zs, axis=0), axis=1, keepdims=True)
        q_pick = jnp.sum(jnp.concatenate(qs, axis=0), axis=1, keepdims=True)
        ratio = jnp.minimum(1.0, jnp.exp(z_pick - m8[bb][:draft, :1]) * i8[bb][:draft, :1] / q_pick)
        picked = jnp.where(lane_b == step * per_step + bb, ratio, picked)
    acc_ref[...] = picked

    for n in range(zb_ref.shape[1] // LANES):
        at = slice(n * LANES, (n + 1) * LANES)
        bon_ref[:, at] = jnp.exp(zb_ref[:, at] - mcol[...]) * icol[...]

    @pl.when(step == pl.num_programs(0) - 1)
    def _():
        run = acc_ref[0:1, :]
        total = run
        for i in range(1, draft):
            run = run * acc_ref[i:i + 1, :]
            total += run
        exp_ref[...] = total


def solution(mesh):
    n_dev = mesh.shape["tp"]

    def local_step(hidden, w_shard, q_rows, x_group):
        seqs, npos, depth = hidden.shape
        seq_dev, draft, vocab = q_rows.shape
        shard = w_shard.shape[1]
        blocks = vocab // LANES
        chips = n_dev // CORES
        seq_chip = seqs // chips
        f32 = jnp.float32
        dma = pltpu.SemaphoreType.DMA
        rows_tile = TILE // LANES * draft
        ksteps = depth // DEPTH
        any_spec = pl.BlockSpec(memory_space=pl.ANY)
        zd, zb, st = pl.pallas_call(
            functools.partial(exchange_kernel, draft, n_dev),
            out_shape=[jax.ShapeDtypeStruct((vocab // TILE, seq_dev * rows_tile, LANES), f32),
                       jax.ShapeDtypeStruct((seq_dev, vocab), f32),
                       jax.ShapeDtypeStruct((n_dev, 16, LANES), f32)],
            in_specs=[any_spec] * 2,
            out_specs=[any_spec] * 3,
            scratch_shapes=[
                pltpu.VMEM((npos, seqs, depth), hidden.dtype),
                pltpu.VMEM((2, depth, TILE), w_shard.dtype),
                pltpu.VMEM((npos * seq_chip, TILE), f32),
                pltpu.VMEM((SLOTS, chips, seq_chip * rows_tile, LANES), f32),
                pltpu.VMEM((SLOTS, chips, seq_chip, TILE), f32),
                pltpu.VMEM((chips, npos, seq_chip, LANES), f32),
                pltpu.VMEM((chips, npos, seq_chip, LANES), f32),
                pltpu.VMEM((chips, CORES, 16, LANES), f32),
                dma((chips, ksteps)), dma((2, ksteps)),
                dma((SLOTS, chips, CORES)), dma((SLOTS, chips, CORES)), dma((chips, CORES)),
                dma((SLOTS,)), dma((SLOTS,)), dma,
                dma((n_dev,)), dma((n_dev,)), dma((n_dev,)),
            ],
            compiler_params=pltpu.CompilerParams(collective_id=0, has_side_effects=True, vmem_limit_bytes=62 * 1024 * 1024),
            cost_estimate=pl.CostEstimate(flops=2 * seqs * npos * depth * shard, bytes_accessed=2 * depth * shard, transcendentals=0),
            name="head_exchange",
        )(hidden.transpose(1, 0, 2), w_shard)

        q3 = q_rows.reshape(seq_dev, draft, blocks, LANES).transpose(0, 2, 1, 3).reshape(seq_dev, blocks * draft, LANES)
        per_step = 4
        steps = seq_dev // per_step
        row_spec = pl.BlockSpec((per_step, blocks * draft, LANES), lambda s: (s, 0, 0))
        z_spec = pl.BlockSpec((vocab // TILE, per_step * rows_tile, LANES), lambda s: (0, s, 0))
        col_spec = pl.BlockSpec((seq_dev, vocab // steps), lambda s: (0, s))
        accept, expected, res, bonus = pl.pallas_call(
            functools.partial(verify_kernel, draft),
            grid=(steps,),
            out_shape=[jax.ShapeDtypeStruct((draft, seq_dev), f32), jax.ShapeDtypeStruct((1, seq_dev), f32),
                       jax.ShapeDtypeStruct((seq_dev, blocks * draft, LANES), f32), jax.ShapeDtypeStruct((seq_dev, vocab), f32)],
            in_specs=[pl.BlockSpec(memory_space=pltpu.SMEM), pl.BlockSpec((n_dev, 16, LANES), lambda s: (0, 0, 0)), z_spec, col_spec, row_spec],
            out_specs=[pl.BlockSpec((draft, seq_dev), lambda s: (0, 0)), pl.BlockSpec((1, seq_dev), lambda s: (0, 0)), row_spec, col_spec],
            scratch_shapes=[pltpu.VMEM((8, LANES), f32), pltpu.VMEM((8, LANES), f32), pltpu.VMEM((seq_dev, LANES), f32), pltpu.VMEM((seq_dev, LANES), f32)],
            compiler_params=pltpu.CompilerParams(dimension_semantics=("arbitrary",), vmem_limit_bytes=62 * 1024 * 1024),
            cost_estimate=pl.CostEstimate(flops=seq_dev * npos * vocab * 8, bytes_accessed=14 * seq_dev * vocab * 4, transcendentals=seq_dev * npos * vocab),
            name="verify_rows",
        )(x_group.T, st, zd, zb, q3)
        residual = res.reshape(seq_dev, blocks, draft, LANES).transpose(0, 2, 1, 3).reshape(seq_dev, draft, vocab)
        return accept.T, expected.reshape(seq_dev), residual, bonus

    return jax.shard_map(local_step, mesh=mesh,
                         in_specs=(P("dp", None, None), P(None, "tp"), P(("dp", "tp"), None, None), P("dp", None)),
                         out_specs=(P(("dp", "tp"), None), P(("dp", "tp")), P(("dp", "tp"), None, None), P(("dp", "tp"), None)),
                         check_vma=False)
```

```python
import functools

import jax
import jax.numpy as jnp
from jax import lax
from jax.experimental import pallas as pl
from jax.experimental.pallas import tpu as pltpu
from jax.sharding import PartitionSpec as P

INV_TEMP = 1.25
LANES = 128
TILE = 256
DEPTH = 2048
SLOTS = 6
CORES = 2
PHASES = 2
UNITS = 2
VMEM_LIMIT = 40 * 1024 * 1024
PEERS = 4


def row_stats(draft, st, seqs):
    m_all = st[:, 0:8, :]
    m = jnp.max(m_all, axis=0)
    inv = 1.0 / jnp.sum(st[:, 8:16, :] * jnp.exp(m_all - m[None]), axis=0)
    rows = [jnp.concatenate([v[:draft], v[:draft]], axis=0) for v in (m, inv)]
    pad = jnp.zeros((LANES - 8, LANES), jnp.float32)
    cols = [jnp.broadcast_to(jnp.concatenate([v, pad], axis=0).T[:seqs, draft:draft + 1], (seqs, LANES)) for v in (m, inv)]
    return rows + cols


def lane_column(rows, lane):
    hit = lax.broadcasted_iota(jnp.int32, (8, LANES), 1) == lane
    return jnp.broadcast_to(jnp.sum(jnp.where(hit, rows, 0.0), axis=1, keepdims=True), (8, LANES))


def inverse_total(draft, total):
    total += pltpu.roll(total, draft, 0)
    return jnp.broadcast_to(1.0 / jnp.sum(total, axis=1, keepdims=True), (8, LANES))


def accept_ratio(draft, tokens, z_row, q_row, m8, i8):
    lane = lax.broadcasted_iota(jnp.int32, (1, LANES), 1)
    zs, qs = [], []
    for i, x in enumerate(tokens):
        pair, half = lax.shift_right_logical(x, 8), lax.shift_right_logical(x, 7) & 1
        hit = lane == (x & (LANES - 1))
        zs.append(jnp.where(hit, z_row(pair, half * draft + i), 0.0))
        qs.append(jnp.where(hit, q_row(pair, half * draft + i), 0.0))
    z = jnp.sum(jnp.concatenate(zs, axis=0), axis=1, keepdims=True)
    q = jnp.sum(jnp.concatenate(qs, axis=0), axis=1, keepdims=True)
    return jnp.minimum(1.0, jnp.exp(z - m8[:draft, :1]) * i8[:draft, :1] / q)


def exchange_kernel(draft, n_dev, h_ref, w_ref, q_ref, x_ref, za_ref, zb_ref, ba_ref, bb_ref, st_ref, acc_ref,
                    hbuf, wbuf, acc, stgd, stgb, mrun, srun, stst, qeven, qodd, mrow, irow, mcol, icol,
                    hsem, wsem, qsem, ssd, ssb, sss, lsd, lsb, lss, rsd, rsb, rss):
    npos = draft + 1
    chips = n_dev // CORES
    seq_dev = h_ref.shape[1] // n_dev
    seq_part = seq_dev // PHASES
    seq_unit = PEERS * seq_part
    depth = h_ref.shape[2]
    depth_steps = depth // DEPTH
    tiles = w_ref.shape[1] // TILE
    lane_blocks = TILE // LANES
    rows_tile = lane_blocks * draft
    me = lax.axis_index("tp")
    chip, core = me // CORES, lax.rem(me, CORES)

    def is_own(u, n):
        return (1 + u + 2 * (n // CORES)) % chips == 0

    def peer(u, n):
        if is_own(u, n):
            return me if n % CORES else me + 1 - 2 * core
        return lax.rem(chip + 1 + u + 2 * (n // CORES), chips) * CORES + n % CORES

    def h_copies(u, p, k):
        cols = pl.ds(pl.multiple_of(k * DEPTH, DEPTH), DEPTH)
        out = []
        for n in range(PEERS):
            rows = pl.ds(pl.multiple_of(peer(u, n) * seq_dev + p * seq_part, seq_part), seq_part)
            out.append(pltpu.make_async_copy(h_ref.at[:, rows, cols], hbuf.at[u, :, n * seq_part:(n + 1) * seq_part, cols], hsem.at[u, n, k]))
        return out

    def w_copy(t, k):
        slot = lax.rem(t, 2)
        rows = pl.ds(pl.multiple_of(k * DEPTH, DEPTH), DEPTH)
        col = pl.multiple_of(lax.rem(t, tiles) * TILE, TILE)
        return pltpu.make_async_copy(w_ref.at[rows, pl.ds(col, TILE)], wbuf.at[slot, rows], wsem.at[slot, k])

    def pieces(t, u, p):
        slot = lax.rem(t, SLOTS)
        block = me * tiles + lax.rem(t, tiles)
        cols = pl.ds(pl.multiple_of(block * TILE, TILE), TILE)
        out = []
        for n in range(PEERS):
            d_src = stgd.at[slot, u, n * seq_part * rows_tile:(n + 1) * seq_part * rows_tile]
            b_src = stgb.at[slot, u, n * seq_part:(n + 1) * seq_part]
            d_dst, b_dst = (za_ref, zb_ref)[p].at[block], (ba_ref, bb_ref)[p].at[:, cols]
            if is_own(u, n) and n % CORES:
                out.append(pltpu.make_async_copy(d_src, d_dst, lsd.at[slot]))
                out.append(pltpu.make_async_copy(b_src, b_dst, lsb.at[slot]))
            else:
                to = {"tp": peer(u, n)}
                out.append(pltpu.make_async_remote_copy(d_src, d_dst, ssd.at[slot, u, n], rsd.at[p, me], device_id=to))
                out.append(pltpu.make_async_remote_copy(b_src, b_dst, ssb.at[slot, u, n], rsb.at[p, me], device_id=to))
        return out

    def stat_pieces(p, u):
        out = []
        for n in range(PEERS):
            src, dst = stst.at[p, u, n], st_ref.at[p, me]
            if is_own(u, n) and n % CORES:
                out.append(pltpu.make_async_copy(src, dst, lss.at[p]))
            else:
                out.append(pltpu.make_async_remote_copy(src, dst, sss.at[p, u, n], rss.at[p, me], device_id={"tp": peer(u, n)}))
        return out

    def wait_sent(copies):
        for copy in copies:
            copy.wait_send() if copy.is_remote else copy.wait()

    def wait_received(p):
        for o in range(1, n_dev):
            src = lax.rem(me + o, n_dev)
            zrows = (za_ref, zb_ref)[p].at[pl.ds(src * tiles, tiles)]
            zcols = (ba_ref, bb_ref)[p].at[:, pl.ds(pl.multiple_of(src * tiles * TILE, TILE), tiles * TILE)]
            pltpu.make_async_copy(zrows, zrows, rsd.at[p, src]).wait()
            pltpu.make_async_copy(zcols, zcols, rsb.at[p, src]).wait()
            pltpu.make_async_copy(st_ref.at[p, src], st_ref.at[p, src], rss.at[p, src]).wait()

    finish_from = tiles + SLOTS + 1

    def q_copy(n, u):
        return pltpu.make_async_copy(q_ref.at[2 * n + u], (qeven, qodd)[u], qsem.at[u])

    def finish(b, q_buf):
        m8, i8 = lane_column(mrow[...], b), lane_column(irow[...], b)
        rows = pl.multiple_of(b * 8, 8)
        first = me * seq_dev + b
        ratio = accept_ratio(draft, [x_ref[i, first] for i in range(draft)],
                             lambda pair, row: za_ref[pair, pl.ds(rows + row, 1), :],
                             lambda pair, row: q_buf[pair, pl.ds(row, 1), :], m8, i8)
        lane = lax.broadcasted_iota(jnp.int32, acc_ref.shape, 1)
        acc_ref[...] = jnp.where(lane == b, ratio, acc_ref[...])
        group = 16
        blocks = za_ref.shape[0]

        def sweep(n, totals):
            totals = list(totals)
            for g in range(group):
                at = n * group + g
                excess = jnp.maximum(jnp.exp(za_ref[at, pl.ds(rows, 8), :] - m8) * i8 - q_buf[at], 0.0)
                za_ref[at, pl.ds(rows, 8), :] = excess
                totals[g % 4] += excess
            return tuple(totals)

        totals = lax.fori_loop(0, blocks // group, sweep, tuple(jnp.zeros((8, LANES), jnp.float32) for _ in range(4)))
        inv = inverse_total(draft, sum(totals))

        def scale(n, carry):
            for g in range(group):
                at = n * group + g
                za_ref[at, pl.ds(rows, 8), :] = za_ref[at, pl.ds(rows, 8), :] * inv
            return carry

        lax.fori_loop(0, blocks // group, scale, 0)
        width = ba_ref.shape[1] // seq_part
        for n in range(width // LANES):
            at = pl.ds(pl.multiple_of(b * width + n * LANES, LANES), LANES)
            ba_ref[:, at] = jnp.exp(ba_ref[:, at] - mcol[...]) * icol[...]

    for k in range(depth_steps):
        for copy in h_copies(0, 0, k):
            copy.start()
        w_copy(0, k).start()

    barrier = pltpu.get_barrier_semaphore()
    for o in range(1, n_dev):
        pl.semaphore_signal(barrier, 1, device_id={"tp": lax.rem(me + o, n_dev)})
    pl.semaphore_wait(barrier, n_dev - 1)

    @pl.loop(0, PHASES * tiles)
    def _(t):
        wslot, slot, p, j = lax.rem(t, 2), lax.rem(t, SLOTS), t // tiles, lax.rem(t, tiles)
        for u in range(UNITS):
            @pl.when(j == 0)
            def _():
                acc[...] = jnp.zeros(acc.shape, jnp.float32)
                mrun[u] = jnp.full(mrun.shape[1:], -jnp.inf, jnp.float32)
                srun[u] = jnp.zeros(srun.shape[1:], jnp.float32)

                @pl.loop(0, depth_steps)
                def _(k):
                    for copy in h_copies(u, p, k):
                        copy.wait()
                    if u + 1 < UNITS:
                        for copy in h_copies(u + 1, p, k):
                            copy.start()
                    if u == 0:
                        w_copy(t, k).wait()
                    else:
                        w_copy(t + 1, k).start()
                    cols = pl.ds(pl.multiple_of(k * DEPTH, DEPTH), DEPTH)
                    acc[...] += jnp.dot(hbuf[u, :, :, cols].reshape(npos * seq_unit, DEPTH), wbuf[wslot, cols, :], preferred_element_type=jnp.float32)

            @pl.when(j > 0)
            def _():
                if u == 0:
                    for k in range(depth_steps):
                        w_copy(t, k).wait()
                else:
                    @pl.when(t + 1 < PHASES * tiles)
                    def _():
                        for k in range(depth_steps):
                            w_copy(t + 1, k).start()
                acc[...] = jnp.dot(hbuf[u].reshape(npos * seq_unit, depth), wbuf[wslot], preferred_element_type=jnp.float32)

            if u == 0:
                @pl.when((j == tiles - 1) & (p + 1 < PHASES))
                def _():
                    for k in range(depth_steps):
                        for copy in h_copies(0, p + 1, k):
                            copy.start()

            @pl.when(t >= SLOTS)
            def _():
                wait_sent(pieces(t - SLOTS, u, 0))

            for i in range(npos):
                zs = [acc[i * seq_unit:(i + 1) * seq_unit, cc * LANES:(cc + 1) * LANES] * INV_TEMP for cc in range(lane_blocks)]
                m_old = mrun[u, i]
                m_new = functools.reduce(jnp.maximum, zs, m_old)
                total = srun[u, i] * jnp.exp(m_old - m_new)
                for cc, z in enumerate(zs):
                    total += jnp.exp(z - m_new)
                    if i < draft:
                        stgd[slot, u, pl.ds(cc * draft + i, seq_unit, stride=rows_tile), :] = z
                    else:
                        stgb[slot, u, :, cc * LANES:(cc + 1) * LANES] = z
                mrun[u, i] = m_new
                srun[u, i] = total
            for static_p in range(PHASES):
                @pl.when(p == static_p)
                def _():
                    for copy in pieces(t, u, static_p):
                        copy.start()

            @pl.when(j == tiles - 1)
            def _():
                lane = lax.broadcasted_iota(jnp.int32, (seq_unit, LANES), 1)
                packed = jnp.zeros((seq_unit, LANES), jnp.float32)
                for i in range(npos):
                    m_lane = mrun[u, i]
                    m = jnp.max(m_lane, axis=1, keepdims=True)
                    s = jnp.sum(srun[u, i] * jnp.exp(m_lane - m), axis=1, keepdims=True)
                    packed = jnp.where(lane == i, m, packed)
                    packed = jnp.where(lane == 8 + i, s, packed)
                flat = jnp.concatenate([packed, jnp.zeros((LANES - seq_unit, LANES), jnp.float32)], axis=0).T[:16]
                for n in range(PEERS):
                    stst[p, u, n] = flat if n == 0 else pltpu.roll(flat, LANES - n * seq_part, 1)
                for copy in stat_pieces(p, u):
                    copy.start()

            @pl.when(t == finish_from - 1)
            def _():
                q_copy(0, u).start()

            @pl.when((t >= finish_from) & (t < finish_from + seq_part // 2))
            def _():
                if u == 0:
                    @pl.when(t == finish_from)
                    def _():
                        for unit in range(UNITS):
                            wait_sent(stat_pieces(0, unit))
                        wait_received(0)
                        for ref, value in zip((mrow, irow, mcol, icol), row_stats(draft, st_ref[0], seq_part)):
                            ref[...] = value
                        acc_ref[...] = jnp.zeros(acc_ref.shape, jnp.float32)
                q_copy(t - finish_from, u).wait()
                finish(2 * (t - finish_from) + u, (qeven, qodd)[u])

                @pl.when(t + 1 < finish_from + seq_part // 2)
                def _():
                    q_copy(t + 1 - finish_from, u).start()

    for t in range(PHASES * tiles - SLOTS, PHASES * tiles):
        for u in range(UNITS):
            wait_sent(pieces(t, u, 1))
    for u in range(UNITS):
        wait_sent(stat_pieces(1, u))
    wait_received(1)


def finish_kernel(draft, x_ref, st_ref, acca_ref, ra_ref, ba_ref, zb_ref, bb_ref, q_ref, acc_ref, exp_ref, res_ref, bon_ref,
                  rb, bonb, mrow, irow, mcol, icol, qsem, rsem, bsem):
    blocks, rows, _ = zb_ref.shape
    seq_part = rows // 8
    group = 4
    first = lax.axis_index("tp") * seq_part * PHASES + seq_part

    def q_copy(b):
        return pltpu.make_async_copy(q_ref.at[seq_part + b], rb.at[b], qsem.at[b])

    def out_copy(b):
        return pltpu.make_async_copy(rb.at[b], res_ref.at[seq_part + b], rsem.at[seq_part + b])

    def out_copy_a(b):
        return pltpu.make_async_copy(ra_ref.at[:, b * 8:(b + 1) * 8], res_ref.at[b], rsem.at[b])

    width = bb_ref.shape[1] // (seq_part // group)

    def bonus_copy(g):
        cols = pl.ds(pl.multiple_of(g * width, width), width)
        return pltpu.make_async_copy(bonb.at[:, cols], bon_ref.at[seq_part:, cols], bsem.at[g + 1])

    bonus_a = pltpu.make_async_copy(ba_ref, bon_ref.at[:seq_part], bsem.at[0])
    for b in range(seq_part):
        q_copy(b).start()
    bonus_a.start()
    for b in range(seq_part):
        out_copy_a(b).start()

    for ref, value in zip((mrow, irow, mcol, icol), row_stats(draft, st_ref[1], seq_part)):
        ref[...] = value
    lane_b = lax.broadcasted_iota(jnp.int32, acc_ref.shape, 1)
    acc_ref[...] = acca_ref[:, :acc_ref.shape[1]]

    @pl.loop(0, seq_part // group)
    def _(g):
        seqs = [g * group + n for n in range(group)]
        m8 = [lane_column(mrow[...], b) for b in seqs]
        i8 = [lane_column(irow[...], b) for b in seqs]
        at_rows = [pl.ds(pl.multiple_of(b * 8, 8), 8) for b in seqs]
        for b in seqs:
            q_copy(b).wait()
        picked = acc_ref[...]
        for n, b in enumerate(seqs):
            ratio = accept_ratio(draft, [x_ref[i, first + b] for i in range(draft)],
                                 lambda pair, row: zb_ref[pair, pl.ds(b * 8 + row, 1), :],
                                 lambda pair, row: rb[b, pair, pl.ds(row, 1), :], m8[n], i8[n])
            picked = jnp.where(lane_b == seq_part + b, ratio, picked)
        acc_ref[...] = picked

        def sweep(k, totals):
            totals = list(totals)
            for n, b in enumerate(seqs):
                for j in range(8):
                    at = k * 8 + j
                    excess = jnp.maximum(jnp.exp(zb_ref[at, at_rows[n], :] - m8[n]) * i8[n] - rb[b, at], 0.0)
                    rb[b, at] = excess
                    totals[n] += excess
            return tuple(totals)

        totals = lax.fori_loop(0, blocks // 8, sweep, tuple(jnp.zeros((8, LANES), jnp.float32) for _ in seqs))
        inv = [inverse_total(draft, total) for total in totals]

        def scale(k, carry):
            for n, b in enumerate(seqs):
                for j in range(8):
                    rb[b, k * 8 + j] = rb[b, k * 8 + j] * inv[n]
            return carry

        lax.fori_loop(0, blocks // 8, scale, 0)
        for b in seqs:
            out_copy(b).start()

        def bonus(k, carry):
            for j in range(8):
                at = pl.ds(pl.multiple_of(g * width + k * 8 * LANES + j * LANES, LANES), LANES)
                bonb[:, at] = jnp.exp(bb_ref[:, at] - mcol[...]) * icol[...]
            return carry

        lax.fori_loop(0, width // (8 * LANES), bonus, 0)
        bonus_copy(g).start()

    run = acc_ref[0:1, :]
    total = run
    for i in range(1, draft):
        run = run * acc_ref[i:i + 1, :]
        total += run
    exp_ref[...] = total

    bonus_a.wait()
    for b in range(seq_part):
        out_copy_a(b).wait()
        out_copy(b).wait()
    for g in range(seq_part // group):
        bonus_copy(g).wait()


def solution(mesh):
    n_dev = mesh.shape["tp"]

    def local_step(hidden, w_shard, q_rows, x_group):
        seqs, npos, depth = hidden.shape
        seq_dev, draft, vocab = q_rows.shape
        shard = w_shard.shape[1]
        blocks = vocab // LANES
        seq_part = seq_dev // PHASES
        seq_unit = PEERS * seq_part
        f32 = jnp.float32
        dma = pltpu.SemaphoreType.DMA
        rows_tile = TILE // LANES * draft
        ksteps = depth // DEPTH
        half_seqs = seq_part * rows_tile
        any_spec = pl.BlockSpec(memory_space=pl.ANY)
        vmem_spec = pl.BlockSpec(memory_space=pltpu.VMEM)
        smem_spec = pl.BlockSpec(memory_space=pltpu.SMEM)
        tokens = x_group.T
        q4 = q_rows.reshape(seq_dev, draft, blocks, LANES).transpose(0, 2, 1, 3).reshape(seq_dev, vocab // TILE, rows_tile, LANES)
        stat_scratch = [pltpu.VMEM((8, LANES), f32)] * 2 + [pltpu.VMEM((seq_part, LANES), f32)] * 2
        res_a, z_b, bon_a, zbon_b, st, acc_a = pl.pallas_call(
            functools.partial(exchange_kernel, draft, n_dev),
            out_shape=[pltpu.VMEM((vocab // TILE, half_seqs, LANES), f32)] * 2 + [pltpu.VMEM((seq_part, vocab), f32)] * 2
                      + [pltpu.VMEM((PHASES, n_dev, 16, LANES), f32), pltpu.VMEM((draft, LANES), f32)],
            in_specs=[any_spec] * 3 + [smem_spec],
            out_specs=[vmem_spec] * 6,
            scratch_shapes=[
                pltpu.VMEM((UNITS, npos, seq_unit, depth), hidden.dtype),
                pltpu.VMEM((2, depth, TILE), w_shard.dtype),
                pltpu.VMEM((npos * seq_unit, TILE), f32),
                pltpu.VMEM((SLOTS, UNITS, seq_unit * rows_tile, LANES), f32),
                pltpu.VMEM((SLOTS, UNITS, seq_unit, TILE), f32),
                pltpu.VMEM((UNITS, npos, seq_unit, LANES), f32),
                pltpu.VMEM((UNITS, npos, seq_unit, LANES), f32),
                pltpu.VMEM((PHASES, UNITS, PEERS, 16, LANES), f32),
                pltpu.VMEM((vocab // TILE, rows_tile, LANES), f32),
                pltpu.VMEM((vocab // TILE, rows_tile, LANES), f32),
                *stat_scratch,
                dma((UNITS, PEERS, ksteps)), dma((2, ksteps)), dma((2,)),
                dma((SLOTS, UNITS, PEERS)), dma((SLOTS, UNITS, PEERS)), dma((PHASES, UNITS, PEERS)),
                dma((SLOTS,)), dma((SLOTS,)), dma((PHASES,)),
                dma((PHASES, n_dev)), dma((PHASES, n_dev)), dma((PHASES, n_dev)),
            ],
            compiler_params=pltpu.CompilerParams(collective_id=0, has_side_effects=True, vmem_limit_bytes=VMEM_LIMIT),
            cost_estimate=pl.CostEstimate(flops=2 * seqs * npos * depth * shard, bytes_accessed=2 * depth * shard, transcendentals=0),
            name="head_exchange",
        )(hidden.transpose(1, 0, 2), w_shard, q4, tokens)

        st, acc_a, res_a, bon_a, z_b, zbon_b = (pltpu.with_memory_space_constraint(v, pltpu.VMEM) for v in (st, acc_a, res_a, bon_a, z_b, zbon_b))
        accept, expected, res, bonus = pl.pallas_call(
            functools.partial(finish_kernel, draft),
            out_shape=[jax.ShapeDtypeStruct((draft, seq_dev), f32), jax.ShapeDtypeStruct((1, seq_dev), f32),
                       jax.ShapeDtypeStruct((seq_dev, vocab // TILE, rows_tile, LANES), f32), jax.ShapeDtypeStruct((seq_dev, vocab), f32)],
            in_specs=[smem_spec] + [vmem_spec] * 6 + [any_spec],
            out_specs=[vmem_spec] * 2 + [any_spec] * 2,
            scratch_shapes=[
                pltpu.VMEM((seq_part, vocab // TILE, rows_tile, LANES), f32), pltpu.VMEM((seq_part, vocab), f32), *stat_scratch,
                dma((seq_part,)), dma((seq_dev,)), dma((seq_part // 4 + 1,)),
            ],
            compiler_params=pltpu.CompilerParams(vmem_limit_bytes=VMEM_LIMIT),
            cost_estimate=pl.CostEstimate(flops=seq_dev * npos * vocab * 8, bytes_accessed=14 * seq_dev * vocab * 4, transcendentals=seq_dev * npos * vocab),
            name="finish_rows",
        )(tokens, st, acc_a, res_a, bon_a, z_b, zbon_b, q4)
        residual = res.reshape(seq_dev, blocks, draft, LANES).transpose(0, 2, 1, 3).reshape(seq_dev, draft, vocab)
        return accept.T, expected.reshape(seq_dev), residual, bonus

    return jax.shard_map(local_step, mesh=mesh,
                         in_specs=(P("dp", None, None), P(None, "tp"), P(("dp", "tp"), None, None), P("dp", None)),
                         out_specs=(P(("dp", "tp"), None), P(("dp", "tp")), P(("dp", "tp"), None, None), P(("dp", "tp"), None)),
                         check_vma=False)
```

```python
import functools

import jax
import jax.numpy as jnp
from jax import lax
from jax.experimental import pallas as pl
from jax.experimental.pallas import tpu as pltpu
from jax.sharding import PartitionSpec as P

INV_TEMP = 1.25
LANES = 128
TILE = 256
DEPTH = 2048
SLOTS = 6
CORES = 2
PHASES = 2
UNITS = 2
VMEM_LIMIT = 35 * 1024 * 1024
PEERS = 4


def row_stats(draft, st, seqs):
    m = functools.reduce(jnp.maximum, st)
    inv = 1.0 / sum(pltpu.roll(part, LANES - seqs, 1) * jnp.exp(part - m) for part in st)
    rows = [jnp.concatenate([v[:draft], v[:draft]], axis=0) for v in (m, inv)]
    pad = jnp.zeros((LANES - 8, LANES), jnp.float32)
    cols = [jnp.broadcast_to(jnp.concatenate([v, pad], axis=0).T[:seqs, draft:draft + 1], (seqs, LANES)) for v in (m, inv)]
    return rows + cols


def lane_column(rows, lane):
    hit = lax.broadcasted_iota(jnp.int32, (8, LANES), 1) == lane
    return jnp.broadcast_to(jnp.sum(jnp.where(hit, rows, 0.0), axis=1, keepdims=True), (8, LANES))


def inverse_total(draft, total):
    total += pltpu.roll(total, draft, 0)
    return jnp.broadcast_to(1.0 / jnp.sum(total, axis=1, keepdims=True), (8, LANES))


def accept_ratio(draft, tokens, z_row, q_row, m8, i8):
    lane = lax.broadcasted_iota(jnp.int32, (1, LANES), 1)
    zs, qs = [], []
    for i, x in enumerate(tokens):
        pair, half = lax.shift_right_logical(x, 8), lax.shift_right_logical(x, 7) & 1
        hit = lane == (x & (LANES - 1))
        zs.append(jnp.where(hit, z_row(pair, half * draft + i), 0.0))
        qs.append(jnp.where(hit, q_row(pair, half * draft + i), 0.0))
    z = jnp.sum(jnp.concatenate(zs, axis=0), axis=1, keepdims=True)
    q = jnp.sum(jnp.concatenate(qs, axis=0), axis=1, keepdims=True)
    return jnp.minimum(1.0, jnp.exp(z - m8[:draft, :1]) * i8[:draft, :1] / q)


def exchange_kernel(draft, n_dev, h_ref, w_ref, q_ref, x_ref, za_ref, zb_ref, qb_ref, st_ref, acc_ref,
                    hbuf, wbuf, acc, stage, mrun, srun, stst, qeven, qodd, mrow, irow, mcol, icol,
                    hsem, wsem, qsem, qbsem, ssd, sss, lsd, lss, rsd, rss):
    npos = draft + 1
    chips = n_dev // CORES
    seq_dev = h_ref.shape[1] // n_dev
    seq_part = seq_dev // PHASES
    seq_unit = PEERS * seq_part
    depth = h_ref.shape[2]
    depth_steps = depth // DEPTH
    tiles = w_ref.shape[1] // TILE
    lane_blocks = TILE // LANES
    rows_tile = lane_blocks * draft
    me = lax.axis_index("tp")
    chip, core = me // CORES, lax.rem(me, CORES)

    def is_own(u, n):
        return (2 - u + 2 * (n // CORES)) % chips == 0

    def peer(u, n):
        if is_own(u, n):
            return me if n % CORES else me + 1 - 2 * core
        return lax.rem(chip + 2 - u + 2 * (n // CORES), chips) * CORES + n % CORES

    def h_copies(u, p, k):
        cols = pl.ds(pl.multiple_of(k * DEPTH, DEPTH), DEPTH)
        out = []
        for n in range(PEERS):
            rows = pl.ds(pl.multiple_of(peer(u, n) * seq_dev + p * seq_part, seq_part), seq_part)
            out.append(pltpu.make_async_copy(h_ref.at[:, rows, cols], hbuf.at[u, :, n * seq_part:(n + 1) * seq_part, cols], hsem.at[u, n, k]))
        return out

    def w_copy(t, k):
        slot = lax.rem(t, 2)
        rows = pl.ds(pl.multiple_of(k * DEPTH, DEPTH), DEPTH)
        col = pl.multiple_of(lax.rem(t, tiles) * TILE, TILE)
        return pltpu.make_async_copy(w_ref.at[rows, pl.ds(col, TILE)], wbuf.at[slot, rows], wsem.at[slot, k])

    def pieces(t, u, p):
        slot = lax.rem(t, SLOTS)
        block = me * tiles + lax.rem(t, tiles)
        out = []
        for n in range(PEERS):
            src, dst = stage.at[slot, u, n], (za_ref, zb_ref)[p].at[block]
            if is_own(u, n) and n % CORES:
                out.append(pltpu.make_async_copy(src, dst, lsd.at[slot]))
            else:
                out.append(pltpu.make_async_remote_copy(src, dst, ssd.at[slot, u, n], rsd.at[p, me], device_id={"tp": peer(u, n)}))
        return out

    def stat_pieces(p, u):
        out = []
        for n in range(PEERS):
            src, dst = stst.at[p, u, n], st_ref.at[p, me]
            if is_own(u, n) and n % CORES:
                out.append(pltpu.make_async_copy(src, dst, lss.at[p]))
            else:
                out.append(pltpu.make_async_remote_copy(src, dst, sss.at[p, u, n], rss.at[p, me], device_id={"tp": peer(u, n)}))
        return out

    def wait_sent(copies):
        for copy in copies:
            copy.wait_send() if copy.is_remote else copy.wait()

    def wait_received(p):
        for o in range(1, n_dev):
            src = lax.rem(me + o, n_dev)
            zrows = (za_ref, zb_ref)[p].at[pl.ds(src * tiles, tiles)]
            pltpu.make_async_copy(zrows, zrows, rsd.at[p, src]).wait()
            pltpu.make_async_copy(st_ref.at[p, src], st_ref.at[p, src], rss.at[p, src]).wait()

    finish_from = tiles + SLOTS + 1

    def q_copy(n, u):
        return pltpu.make_async_copy(q_ref.at[2 * n + u], (qeven, qodd)[u], qsem.at[u])

    def qb_copy(b):
        return pltpu.make_async_copy(q_ref.at[seq_part + b], qb_ref.at[b], qbsem.at[b])

    def finish(b, q_buf):
        m8, i8 = lane_column(mrow[...], b), lane_column(irow[...], b)
        rows = pl.multiple_of(b * 8, 8)
        first = me * seq_dev + b
        ratio = accept_ratio(draft, [x_ref[i, first] for i in range(draft)],
                             lambda pair, row: za_ref[pair, pl.ds(rows + row, 1), :],
                             lambda pair, row: q_buf[pair, pl.ds(row, 1), :], m8, i8)
        lane = lax.broadcasted_iota(jnp.int32, acc_ref.shape, 1)
        acc_ref[...] = jnp.where(lane == b, ratio, acc_ref[...])
        group = 16
        blocks = za_ref.shape[0]

        def sweep(n, totals):
            totals = list(totals)
            for g in range(group):
                at = n * group + g
                excess = jnp.maximum(jnp.exp(za_ref[at, pl.ds(rows, 8), :] - m8) * i8 - q_buf[at], 0.0)
                za_ref[at, pl.ds(rows, 8), :] = excess
                totals[g % 4] += excess
            return tuple(totals)

        totals = lax.fori_loop(0, blocks // group, sweep, tuple(jnp.zeros((8, LANES), jnp.float32) for _ in range(4)))
        inv = inverse_total(draft, sum(totals))

        def scale(n, carry):
            for g in range(group):
                at = n * group + g
                za_ref[at, pl.ds(rows, 8), :] = za_ref[at, pl.ds(rows, 8), :] * inv
            return carry

        lax.fori_loop(0, blocks // group, scale, 0)
        part = blocks // seq_part
        for n in range(part):
            for row in range(0, seq_part, 8):
                for cc in range(lane_blocks):
                    at = pl.ds(seq_part * rows_tile + row * lane_blocks + cc * 8, 8)
                    za_ref[b * part + n, at, :] = jnp.exp(za_ref[b * part + n, at, :] - mcol[row:row + 8]) * icol[row:row + 8]

    for k in range(depth_steps):
        for copy in h_copies(0, 0, k):
            copy.start()
        w_copy(0, k).start()

    barrier = pltpu.get_barrier_semaphore()
    for o in range(1, n_dev):
        pl.semaphore_signal(barrier, 1, device_id={"tp": lax.rem(me + o, n_dev)})
    pl.semaphore_wait(barrier, n_dev - 1)

    @pl.loop(0, PHASES * tiles)
    def _(t):
        wslot, slot, p, j = lax.rem(t, 2), lax.rem(t, SLOTS), t // tiles, lax.rem(t, tiles)
        for u in range(UNITS):
            @pl.when(j == 0)
            def _():
                acc[...] = jnp.zeros(acc.shape, jnp.float32)
                mrun[u] = jnp.full(mrun.shape[1:], -jnp.inf, jnp.float32)
                srun[u] = jnp.zeros(srun.shape[1:], jnp.float32)

                @pl.loop(0, depth_steps)
                def _(k):
                    for copy in h_copies(u, p, k):
                        copy.wait()
                    if u + 1 < UNITS:
                        for copy in h_copies(u + 1, p, k):
                            copy.start()
                    if u == 0:
                        w_copy(t, k).wait()
                    else:
                        w_copy(t + 1, k).start()
                    cols = pl.ds(pl.multiple_of(k * DEPTH, DEPTH), DEPTH)
                    acc[...] += jnp.dot(hbuf[u, :, :, cols].reshape(npos * seq_unit, DEPTH), wbuf[wslot, cols, :], preferred_element_type=jnp.float32)

            @pl.when(j > 0)
            def _():
                if u == 0:
                    for k in range(depth_steps):
                        w_copy(t, k).wait()
                else:
                    @pl.when(t + 1 < PHASES * tiles)
                    def _():
                        for k in range(depth_steps):
                            w_copy(t + 1, k).start()
                acc[...] = jnp.dot(hbuf[u].reshape(npos * seq_unit, depth), wbuf[wslot], preferred_element_type=jnp.float32)

            if u == 0:
                @pl.when((j == tiles - 1) & (p + 1 < PHASES))
                def _():
                    for k in range(depth_steps):
                        for copy in h_copies(0, p + 1, k):
                            copy.start()

            @pl.when(t >= SLOTS)
            def _():
                wait_sent(pieces(t - SLOTS, u, 0))

            for i in range(npos):
                zs = [acc[i * seq_unit:(i + 1) * seq_unit, cc * LANES:(cc + 1) * LANES] * INV_TEMP for cc in range(lane_blocks)]
                m_old = mrun[u, i]
                m_new = functools.reduce(jnp.maximum, zs, m_old)
                total = srun[u, i] * jnp.exp(m_old - m_new)
                for cc, z in enumerate(zs):
                    total += jnp.exp(z - m_new)
                    for n in range(PEERS):
                        z_n = z[n * seq_part:(n + 1) * seq_part]
                        if i < draft:
                            stage[slot, u, n, pl.ds(cc * draft + i, seq_part, stride=rows_tile), :] = z_n
                        else:
                            for row in range(0, seq_part, 8):
                                at = seq_part * rows_tile + row * lane_blocks + cc * 8
                                stage[slot, u, n, at:at + 8, :] = z_n[row:row + 8]
                mrun[u, i] = m_new
                srun[u, i] = total
            for static_p in range(PHASES):
                @pl.when(p == static_p)
                def _():
                    for copy in pieces(t, u, static_p):
                        copy.start()

            @pl.when(j == tiles - 1)
            def _():
                lane = lax.broadcasted_iota(jnp.int32, (seq_unit, LANES), 1)
                packed = jnp.zeros((seq_unit, LANES), jnp.float32)
                for i in range(npos):
                    m_lane = mrun[u, i]
                    m = jnp.max(m_lane, axis=1, keepdims=True)
                    s = jnp.sum(srun[u, i] * jnp.exp(m_lane - m), axis=1, keepdims=True)
                    packed = jnp.where(lane == i, m, packed)
                    packed = jnp.where(lane == 8 + i, s, packed)
                flat = jnp.concatenate([packed, jnp.zeros((LANES - seq_unit, LANES), jnp.float32)], axis=0).T[:16]
                for n in range(PEERS):
                    m_n, s_n = (pltpu.roll(v, (LANES - n * seq_part + shift) % LANES, 1) for v, shift in ((flat[:8], 0), (flat[8:], seq_part)))
                    stst[p, u, n] = jnp.where(lane[:8] < seq_part, m_n, s_n)
                for copy in stat_pieces(p, u):
                    copy.start()

            if u == 0:
                @pl.when((t >= tiles) & (t < tiles + seq_part))
                def _():
                    qb_copy(t - tiles).start()

            @pl.when(t == finish_from - 1)
            def _():
                q_copy(0, u).start()

            @pl.when((t >= finish_from) & (t < finish_from + seq_part // 2))
            def _():
                if u == 0:
                    @pl.when(t == finish_from)
                    def _():
                        for unit in range(UNITS):
                            wait_sent(stat_pieces(0, unit))
                        wait_received(0)
                        for ref, value in zip((mrow, irow, mcol, icol), row_stats(draft, [st_ref[0, n] for n in range(n_dev)], seq_part)):
                            ref[...] = value
                        acc_ref[...] = jnp.zeros(acc_ref.shape, jnp.float32)
                q_copy(t - finish_from, u).wait()
                finish(2 * (t - finish_from) + u, (qeven, qodd)[u])

                @pl.when(t + 1 < finish_from + seq_part // 2)
                def _():
                    q_copy(t + 1 - finish_from, u).start()

    for t in range(PHASES * tiles - SLOTS, PHASES * tiles):
        for u in range(UNITS):
            wait_sent(pieces(t, u, 1))
    for u in range(UNITS):
        wait_sent(stat_pieces(1, u))
    for b in range(seq_part):
        qb_copy(b).wait()
    wait_received(1)


def finish_kernel(draft, x_ref, st_ref, acca_ref, ra_ref, zb_ref, q_ref, acc_ref, exp_ref, res_ref, bon_ref,
                  rb, bonb, mrow, irow, mcol, icol, rsem, bsem):
    blocks = zb_ref.shape[0]
    seq_part, _, rows_tile, _ = q_ref.shape
    lane_blocks = rows_tile // draft
    strips = seq_part // 8
    group = 4
    first = lax.axis_index("tp") * seq_part * PHASES + seq_part

    def out_copy(b):
        return pltpu.make_async_copy(rb.at[b], res_ref.at[seq_part + b], rsem.at[seq_part + b])

    def out_copy_a(b):
        return pltpu.make_async_copy(ra_ref.at[:, b * 8:(b + 1) * 8], res_ref.at[b], rsem.at[b])

    def strip(n):
        at = seq_part * rows_tile + n * lane_blocks * 8
        return slice(at, at + lane_blocks * 8)

    def bonus_copy_a(n):
        return pltpu.make_async_copy(ra_ref.at[:, strip(n)], bon_ref.at[n], bsem.at[n])

    width = blocks // (seq_part // group)

    def bonus_copy(g):
        at = pl.ds(g * width, width)
        return pltpu.make_async_copy(bonb.at[:, at], bon_ref.at[strips:, at], bsem.at[strips + g])

    for b in range(seq_part):
        out_copy_a(b).start()
    for n in range(strips):
        bonus_copy_a(n).start()

    for ref, value in zip((mrow, irow, mcol, icol), row_stats(draft, [st_ref[1, n] for n in range(st_ref.shape[1])], seq_part)):
        ref[...] = value
    lane_b = lax.broadcasted_iota(jnp.int32, acc_ref.shape, 1)
    acc_ref[...] = acca_ref[:, :acc_ref.shape[1]]

    @pl.loop(0, seq_part // group)
    def _(g):
        seqs = [g * group + n for n in range(group)]
        m8 = [lane_column(mrow[...], b) for b in seqs]
        i8 = [lane_column(irow[...], b) for b in seqs]
        at_rows = [pl.ds(pl.multiple_of(b * 8, 8), 8) for b in seqs]
        picked = acc_ref[...]
        for n, b in enumerate(seqs):
            ratio = accept_ratio(draft, [x_ref[i, first + b] for i in range(draft)],
                                 lambda pair, row: zb_ref[pair, pl.ds(b * 8 + row, 1), :],
                                 lambda pair, row: q_ref[b, pair, pl.ds(row, 1), :], m8[n], i8[n])
            picked = jnp.where(lane_b == seq_part + b, ratio, picked)
        acc_ref[...] = picked

        def sweep(k, totals):
            totals = list(totals)
            for n, b in enumerate(seqs):
                for j in range(8):
                    at = k * 8 + j
                    excess = jnp.maximum(jnp.exp(zb_ref[at, at_rows[n], :] - m8[n]) * i8[n] - q_ref[b, at], 0.0)
                    rb[b, at] = excess
                    totals[n] += excess
            return tuple(totals)

        totals = lax.fori_loop(0, blocks // 8, sweep, tuple(jnp.zeros((8, LANES), jnp.float32) for _ in seqs))
        inv = [inverse_total(draft, total) for total in totals]

        def scale(k, carry):
            for n, b in enumerate(seqs):
                for j in range(8):
                    rb[b, k * 8 + j] = rb[b, k * 8 + j] * inv[n]
            return carry

        lax.fori_loop(0, blocks // 8, scale, 0)
        for b in seqs:
            out_copy(b).start()

        def bonus(k, carry):
            at = g * width + k
            for n in range(strips):
                for cc in range(lane_blocks):
                    row = strip(n).start + cc * 8
                    seqs8 = slice(n * 8, (n + 1) * 8)
                    bonb[n, at, cc * 8:(cc + 1) * 8, :] = jnp.exp(zb_ref[at, row:row + 8, :] - mcol[seqs8]) * icol[seqs8]
            return carry

        lax.fori_loop(0, width, bonus, 0, unroll=4)
        bonus_copy(g).start()

    run = acc_ref[0:1, :]
    total = run
    for i in range(1, draft):
        run = run * acc_ref[i:i + 1, :]
        total += run
    exp_ref[...] = total

    for n in range(strips):
        bonus_copy_a(n).wait()
    for b in range(seq_part):
        out_copy_a(b).wait()
        out_copy(b).wait()
    for g in range(seq_part // group):
        bonus_copy(g).wait()


def solution(mesh):
    n_dev = mesh.shape["tp"]

    def local_step(hidden, w_shard, q_rows, x_group):
        seqs, npos, depth = hidden.shape
        seq_dev, draft, vocab = q_rows.shape
        shard = w_shard.shape[1]
        blocks = vocab // LANES
        seq_part = seq_dev // PHASES
        seq_unit = PEERS * seq_part
        f32 = jnp.float32
        dma = pltpu.SemaphoreType.DMA
        rows_tile = TILE // LANES * draft
        ksteps = depth // DEPTH
        rows_block = seq_part * (rows_tile + TILE // LANES)
        any_spec = pl.BlockSpec(memory_space=pl.ANY)
        vmem_spec = pl.BlockSpec(memory_space=pltpu.VMEM)
        smem_spec = pl.BlockSpec(memory_space=pltpu.SMEM)
        tokens = x_group.T
        q4 = q_rows.reshape(seq_dev, draft, blocks, LANES).transpose(0, 2, 1, 3).reshape(seq_dev, vocab // TILE, rows_tile, LANES)
        stat_scratch = [pltpu.VMEM((8, LANES), f32)] * 2 + [pltpu.VMEM((seq_part, LANES), f32)] * 2
        res_a, z_b, q_b, st, acc_a = pl.pallas_call(
            functools.partial(exchange_kernel, draft, n_dev),
            out_shape=[pltpu.VMEM((vocab // TILE, rows_block, LANES), f32)] * 2 + [pltpu.VMEM((seq_part, vocab // TILE, rows_tile, LANES), f32)]
                      + [pltpu.VMEM((PHASES, n_dev, 8, LANES), f32), pltpu.VMEM((draft, LANES), f32)],
            in_specs=[any_spec] * 3 + [smem_spec],
            out_specs=[vmem_spec] * 5,
            scratch_shapes=[
                pltpu.VMEM((UNITS, npos, seq_unit, depth), hidden.dtype),
                pltpu.VMEM((2, depth, TILE), w_shard.dtype),
                pltpu.VMEM((npos * seq_unit, TILE), f32),
                pltpu.VMEM((SLOTS, UNITS, PEERS, rows_block, LANES), f32),
                pltpu.VMEM((UNITS, npos, seq_unit, LANES), f32),
                pltpu.VMEM((UNITS, npos, seq_unit, LANES), f32),
                pltpu.VMEM((PHASES, UNITS, PEERS, 8, LANES), f32),
                pltpu.VMEM((vocab // TILE, rows_tile, LANES), f32),
                pltpu.VMEM((vocab // TILE, rows_tile, LANES), f32),
                *stat_scratch,
                dma((UNITS, PEERS, ksteps)), dma((2, ksteps)), dma((2,)), dma((seq_part,)),
                dma((SLOTS, UNITS, PEERS)), dma((PHASES, UNITS, PEERS)), dma((SLOTS,)), dma((PHASES,)),
                dma((PHASES, n_dev)), dma((PHASES, n_dev)),
            ],
            compiler_params=pltpu.CompilerParams(collective_id=0, has_side_effects=True, vmem_limit_bytes=VMEM_LIMIT),
            cost_estimate=pl.CostEstimate(flops=2 * seqs * npos * depth * shard, bytes_accessed=2 * depth * shard, transcendentals=0),
            name="head_exchange",
        )(hidden.transpose(1, 0, 2), w_shard, q4, tokens)

        st, acc_a, res_a, z_b, q_b = (pltpu.with_memory_space_constraint(v, pltpu.VMEM) for v in (st, acc_a, res_a, z_b, q_b))
        accept, expected, res, bonus = pl.pallas_call(
            functools.partial(finish_kernel, draft),
            out_shape=[jax.ShapeDtypeStruct((draft, seq_dev), f32), jax.ShapeDtypeStruct((1, seq_dev), f32),
                       jax.ShapeDtypeStruct((seq_dev, vocab // TILE, rows_tile, LANES), f32),
                       jax.ShapeDtypeStruct((seq_dev // 8, vocab // TILE, TILE // LANES * 8, LANES), f32)],
            in_specs=[smem_spec] + [vmem_spec] * 5,
            out_specs=[vmem_spec] * 2 + [any_spec] * 2,
            scratch_shapes=[
                pltpu.VMEM((seq_part, vocab // TILE, rows_tile, LANES), f32), pltpu.VMEM((seq_part // 8, vocab // TILE, TILE // LANES * 8, LANES), f32), *stat_scratch,
                dma((seq_dev,)), dma((seq_part // 8 + seq_part // 4,)),
            ],
            compiler_params=pltpu.CompilerParams(vmem_limit_bytes=VMEM_LIMIT),
            cost_estimate=pl.CostEstimate(flops=seq_dev * npos * vocab * 8, bytes_accessed=14 * seq_dev * vocab * 4, transcendentals=seq_dev * npos * vocab),
            name="finish_rows",
        )(tokens, st, acc_a, res_a, z_b, q_b)
        residual = res.reshape(seq_dev, blocks, draft, LANES).transpose(0, 2, 1, 3).reshape(seq_dev, draft, vocab)
        return accept.T, expected.reshape(seq_dev), residual, bonus.reshape(seq_dev // 8, vocab // TILE, TILE // LANES, 8, LANES).transpose(0, 3, 1, 2, 4).reshape(seq_dev, vocab)

    return jax.shard_map(local_step, mesh=mesh,
                         in_specs=(P("dp", None, None), P(None, "tp"), P(("dp", "tp"), None, None), P("dp", None)),
                         out_specs=(P(("dp", "tp"), None), P(("dp", "tp")), P(("dp", "tp"), None, None), P(("dp", "tp"), None)),
                         check_vma=False)
```

```python
import functools

import jax
import jax.numpy as jnp
from jax import lax
from jax.experimental import pallas as pl
from jax.experimental.pallas import tpu as pltpu
from jax.sharding import PartitionSpec as P

INV_TEMP = 1.25
LANES = 128
TILE = 256
DEPTH = 3072
SLOTS = 6
CORES = 2
PHASES = 2
UNITS = 2
VMEM_LIMIT = 35 * 1024 * 1024
PEERS = 4


def row_stats(draft, st, seqs):
    m = functools.reduce(jnp.maximum, st)
    inv = 1.0 / sum(pltpu.roll(part, LANES - seqs, 1) * jnp.exp(part - m) for part in st)
    rows = [jnp.concatenate([v[:draft], v[:draft]], axis=0) for v in (m, inv)]
    pad = jnp.zeros((LANES - 8, LANES), jnp.float32)
    cols = [jnp.broadcast_to(jnp.concatenate([v, pad], axis=0).T[:seqs, draft:draft + 1], (seqs, LANES)) for v in (m, inv)]
    return rows + cols


def lane_column(rows, lane):
    hit = lax.broadcasted_iota(jnp.int32, (8, LANES), 1) == lane
    return jnp.broadcast_to(jnp.sum(jnp.where(hit, rows, 0.0), axis=1, keepdims=True), (8, LANES))


def inverse_total(draft, total):
    total += pltpu.roll(total, draft, 0)
    return jnp.broadcast_to(1.0 / jnp.sum(total, axis=1, keepdims=True), (8, LANES))


def accept_ratio(draft, tokens, z_row, q_row, m8, i8):
    lane = lax.broadcasted_iota(jnp.int32, (1, LANES), 1)
    zs, qs = [], []
    for i, x in enumerate(tokens):
        pair, half = lax.shift_right_logical(x, 8), lax.shift_right_logical(x, 7) & 1
        hit = lane == (x & (LANES - 1))
        zs.append(jnp.where(hit, z_row(pair, half * draft + i), 0.0))
        qs.append(jnp.where(hit, q_row(pair, half * draft + i), 0.0))
    z = jnp.sum(jnp.concatenate(zs, axis=0), axis=1, keepdims=True)
    q = jnp.sum(jnp.concatenate(qs, axis=0), axis=1, keepdims=True)
    return jnp.minimum(1.0, jnp.exp(z - m8[:draft, :1]) * i8[:draft, :1] / q)


def exchange_kernel(draft, n_dev, h_ref, w_ref, q_ref, x_ref, za_ref, zb_ref, qb_ref, st_ref, acc_ref,
                    hbuf, wbuf, acc, stage, mrun, srun, stst, qeven, qodd, mrow, irow, mcol, icol,
                    hsem, wsem, qsem, qbsem, ssd, sss, lsd, lss, rsd, rss):
    npos = draft + 1
    chips = n_dev // CORES
    seq_dev = h_ref.shape[1] // n_dev
    seq_part = seq_dev // PHASES
    seq_unit = PEERS * seq_part
    depth = h_ref.shape[2]
    depth_steps = depth // DEPTH
    tiles = w_ref.shape[1] // TILE
    lane_blocks = TILE // LANES
    rows_tile = lane_blocks * draft
    me = lax.axis_index("tp")
    chip, core = me // CORES, lax.rem(me, CORES)

    def is_own(u, n):
        return (2 - u + 2 * (n // CORES)) % chips == 0

    def peer(u, n):
        if is_own(u, n):
            return me if n % CORES else me + 1 - 2 * core
        return lax.rem(chip + 2 - u + 2 * (n // CORES), chips) * CORES + n % CORES

    def h_copies(u, p, k, peers):
        cols = pl.ds(pl.multiple_of(k * DEPTH, DEPTH), DEPTH)
        out = []
        for n in peers:
            rows = pl.ds(pl.multiple_of(peer(u, n) * seq_dev + p * seq_part, seq_part), seq_part)
            out.append(pltpu.make_async_copy(h_ref.at[:, rows, cols], hbuf.at[u, :, n * seq_part:(n + 1) * seq_part, cols], hsem.at[u, n, k]))
        return out

    def w_copy(t, k):
        slot = lax.rem(t, 2)
        rows = pl.ds(pl.multiple_of(k * DEPTH, DEPTH), DEPTH)
        col = pl.multiple_of(lax.rem(t, tiles) * TILE, TILE)
        return pltpu.make_async_copy(w_ref.at[rows, pl.ds(col, TILE)], wbuf.at[slot, rows], wsem.at[slot, k])

    def pieces(t, u, p, peers):
        slot = lax.rem(t, SLOTS)
        block = me * tiles + lax.rem(t, tiles)
        out = []
        for n in peers:
            src, dst = stage.at[slot, u, n], (za_ref, zb_ref)[p].at[block]
            if is_own(u, n) and n % CORES:
                out.append(pltpu.make_async_copy(src, dst, lsd.at[slot]))
            else:
                out.append(pltpu.make_async_remote_copy(src, dst, ssd.at[slot, u, n], rsd.at[p, me], device_id={"tp": peer(u, n)}))
        return out

    def stat_pieces(p, u):
        out = []
        for n in range(PEERS):
            src, dst = stst.at[p, u, n], st_ref.at[p, me]
            if is_own(u, n) and n % CORES:
                out.append(pltpu.make_async_copy(src, dst, lss.at[p]))
            else:
                out.append(pltpu.make_async_remote_copy(src, dst, sss.at[p, u, n], rss.at[p, me], device_id={"tp": peer(u, n)}))
        return out

    def wait_sent(copies):
        for copy in copies:
            copy.wait_send() if copy.is_remote else copy.wait()

    def wait_received(p):
        for o in range(1, n_dev):
            src = lax.rem(me + o, n_dev)
            zrows = (za_ref, zb_ref)[p].at[pl.ds(src * tiles, tiles)]
            pltpu.make_async_copy(zrows, zrows, rsd.at[p, src]).wait()
            pltpu.make_async_copy(st_ref.at[p, src], st_ref.at[p, src], rss.at[p, src]).wait()

    finish_from = tiles + SLOTS + 1

    def q_copy(n, u):
        return pltpu.make_async_copy(q_ref.at[2 * n + u], (qeven, qodd)[u], qsem.at[u])

    def qb_copy(b):
        return pltpu.make_async_copy(q_ref.at[seq_part + b], qb_ref.at[b], qbsem.at[b])

    def finish(b, q_buf):
        m8, i8 = lane_column(mrow[...], b), lane_column(irow[...], b)
        rows = pl.multiple_of(b * 8, 8)
        first = me * seq_dev + b
        ratio = accept_ratio(draft, [x_ref[i, first] for i in range(draft)],
                             lambda pair, row: za_ref[pair, pl.ds(rows + row, 1), :],
                             lambda pair, row: q_buf[pair, pl.ds(row, 1), :], m8, i8)
        lane = lax.broadcasted_iota(jnp.int32, acc_ref.shape, 1)
        acc_ref[...] = jnp.where(lane == b, ratio, acc_ref[...])
        group = 16
        blocks = za_ref.shape[0]

        def sweep(n, totals):
            totals = list(totals)
            for g in range(group):
                at = n * group + g
                excess = jnp.maximum(jnp.exp(za_ref[at, pl.ds(rows, 8), :] - m8) * i8 - q_buf[at], 0.0)
                za_ref[at, pl.ds(rows, 8), :] = excess
                totals[g % 4] += excess
            return tuple(totals)

        totals = lax.fori_loop(0, blocks // group, sweep, tuple(jnp.zeros((8, LANES), jnp.float32) for _ in range(4)))
        inv = inverse_total(draft, sum(totals))

        def scale(n, carry):
            for g in range(group):
                at = n * group + g
                za_ref[at, pl.ds(rows, 8), :] = za_ref[at, pl.ds(rows, 8), :] * inv
            return carry

        lax.fori_loop(0, blocks // group, scale, 0)
        part = blocks // seq_part
        for n in range(part):
            for row in range(0, seq_part, 8):
                for cc in range(lane_blocks):
                    at = pl.ds(seq_part * rows_tile + row * lane_blocks + cc * 8, 8)
                    za_ref[b * part + n, at, :] = jnp.exp(za_ref[b * part + n, at, :] - mcol[row:row + 8]) * icol[row:row + 8]

    everyone, far, own = tuple(range(PEERS)), tuple(range(CORES)), tuple(range(CORES, PEERS))
    last = PHASES * tiles - 1

    def start_all(copies):
        for copy in copies:
            copy.start()

    for k in range(depth_steps):
        start_all(h_copies(0, 0, k, far))
        w_copy(0, k).start()

    barrier = pltpu.get_barrier_semaphore()
    for o in range(1, n_dev):
        pl.semaphore_signal(barrier, 1, device_id={"tp": lax.rem(me + o, n_dev)})
    pl.semaphore_wait(barrier, n_dev - 1)

    def multiply_as_it_comes(t, u, peers):
        p = t // tiles
        rows = slice(peers[0] * seq_part, (peers[-1] + 1) * seq_part)
        count = len(peers) * seq_part
        acc[:, rows, :] = jnp.zeros((npos, count, TILE), jnp.float32)
        mrun[u] = jnp.full(mrun.shape[1:], -jnp.inf, jnp.float32)
        srun[u] = jnp.zeros(srun.shape[1:], jnp.float32)

        @pl.loop(0, depth_steps)
        def _(k):
            for copy in h_copies(u, p, k, peers):
                copy.wait()
            if peers == far:
                w_copy(t, k).wait()
                start_all(h_copies(1, p, k, everyone))
            else:
                start_all(h_copies(0, p, k, own))
                w_copy(t + 1, k).start()
            cols = pl.ds(pl.multiple_of(k * DEPTH, DEPTH), DEPTH)
            lhs = hbuf[u, :, rows, cols].reshape(npos * count, DEPTH)
            prod = jnp.dot(lhs, wbuf[lax.rem(t, 2), cols, :], preferred_element_type=jnp.float32)
            acc[:, rows, :] += prod.reshape(npos, count, TILE)

    def multiply(t, u):
        if u == 0:
            for k in range(depth_steps):
                w_copy(t, k).wait()
        else:
            @pl.when(t < last)
            def _():
                for k in range(depth_steps):
                    w_copy(t + 1, k).start()
        prod = jnp.dot(hbuf[u].reshape(npos * seq_unit, depth), wbuf[lax.rem(t, 2)], preferred_element_type=jnp.float32)
        acc[...] = prod.reshape(acc.shape)

    def multiply_own(t):
        rows = slice(CORES * seq_part, seq_unit)
        count = seq_unit - CORES * seq_part
        prod = jnp.dot(hbuf[0, :, rows].reshape(npos * count, depth), wbuf[lax.rem(t, 2)], preferred_element_type=jnp.float32)
        acc[:, rows, :] = prod.reshape(npos, count, TILE)

    def send(t, u, peers):
        slot, p = lax.rem(t, SLOTS), t // tiles

        @pl.when(t >= SLOTS)
        def _():
            wait_sent(pieces(t - SLOTS, u, 0, peers))

        rows = slice(peers[0] * seq_part, (peers[-1] + 1) * seq_part)
        for i in range(npos):
            zs = [acc[i, rows, cc * LANES:(cc + 1) * LANES] * INV_TEMP for cc in range(lane_blocks)]
            m_old = mrun[u, i, rows]
            m_new = functools.reduce(jnp.maximum, zs, m_old)
            total = srun[u, i, rows] * jnp.exp(m_old - m_new)
            for cc, z in enumerate(zs):
                total += jnp.exp(z - m_new)
                for at_n, n in enumerate(peers):
                    z_n = z[at_n * seq_part:(at_n + 1) * seq_part]
                    if i < draft:
                        stage[slot, u, n, pl.ds(cc * draft + i, seq_part, stride=rows_tile), :] = z_n
                    else:
                        for row in range(0, seq_part, 8):
                            at = seq_part * rows_tile + row * lane_blocks + cc * 8
                            stage[slot, u, n, at:at + 8, :] = z_n[row:row + 8]
            mrun[u, i, rows] = m_new
            srun[u, i, rows] = total
        for static_p in range(PHASES):
            @pl.when(p == static_p)
            def _():
                start_all(pieces(t, u, static_p, peers))

    @pl.loop(0, PHASES * tiles)
    def _(t):
        p, j = t // tiles, lax.rem(t, tiles)
        for u in range(UNITS):
            peers = far if u == 0 else everyone

            @pl.when(j == 0)
            def _():
                multiply_as_it_comes(t, u, peers)

            if u == 0:
                @pl.when(j == 1)
                def _():
                    for k in range(depth_steps):
                        for copy in h_copies(0, p, k, own):
                            copy.wait()

            @pl.when(j > 0)
            def _():
                multiply(t, u)

            if u == 0:
                @pl.when((j == tiles - 1) & (p + 1 < PHASES))
                def _():
                    for k in range(depth_steps):
                        start_all(h_copies(0, p + 1, k, far))

            send(t, u, peers)
            if u == 0:
                @pl.when(j > 0)
                def _():
                    send(t, 0, own)

                @pl.when(j == 1)
                def _():
                    multiply_own(t - 1)
                    send(t - 1, 0, own)

            @pl.when(j == tiles - 1)
            def _():
                lane = lax.broadcasted_iota(jnp.int32, (seq_unit, LANES), 1)
                packed = jnp.zeros((seq_unit, LANES), jnp.float32)
                for i in range(npos):
                    m_lane = mrun[u, i]
                    m = jnp.max(m_lane, axis=1, keepdims=True)
                    s = jnp.sum(srun[u, i] * jnp.exp(m_lane - m), axis=1, keepdims=True)
                    packed = jnp.where(lane == i, m, packed)
                    packed = jnp.where(lane == 8 + i, s, packed)
                flat = jnp.concatenate([packed, jnp.zeros((LANES - seq_unit, LANES), jnp.float32)], axis=0).T[:16]
                for n in range(PEERS):
                    m_n, s_n = (pltpu.roll(v, (LANES - n * seq_part + shift) % LANES, 1) for v, shift in ((flat[:8], 0), (flat[8:], seq_part)))
                    stst[p, u, n] = jnp.where(lane[:8] < seq_part, m_n, s_n)
                for copy in stat_pieces(p, u):
                    copy.start()

            if u == 0:
                @pl.when((t >= tiles) & (t < tiles + seq_part))
                def _():
                    qb_copy(t - tiles).start()

            @pl.when(t == finish_from - 1)
            def _():
                q_copy(0, u).start()

            @pl.when((t >= finish_from) & (t < finish_from + seq_part // 2))
            def _():
                if u == 0:
                    @pl.when(t == finish_from)
                    def _():
                        for unit in range(UNITS):
                            wait_sent(stat_pieces(0, unit))
                        wait_received(0)
                        for ref, value in zip((mrow, irow, mcol, icol), row_stats(draft, [st_ref[0, n] for n in range(n_dev)], seq_part)):
                            ref[...] = value
                        acc_ref[...] = jnp.zeros(acc_ref.shape, jnp.float32)
                q_copy(t - finish_from, u).wait()
                finish(2 * (t - finish_from) + u, (qeven, qodd)[u])

                @pl.when(t + 1 < finish_from + seq_part // 2)
                def _():
                    q_copy(t + 1 - finish_from, u).start()

    for t in range(PHASES * tiles - SLOTS, PHASES * tiles):
        for u in range(UNITS):
            wait_sent(pieces(t, u, 1, everyone))
    for u in range(UNITS):
        wait_sent(stat_pieces(1, u))
    for b in range(seq_part):
        qb_copy(b).wait()
    wait_received(1)


def finish_kernel(draft, x_ref, st_ref, acca_ref, ra_ref, zb_ref, q_ref, acc_ref, exp_ref, res_ref, bon_ref,
                  rb, bonb, mrow, irow, mcol, icol, rsem, bsem):
    blocks = zb_ref.shape[0]
    seq_part, _, rows_tile, _ = q_ref.shape
    lane_blocks = rows_tile // draft
    strips = seq_part // 8
    group = 4
    first = lax.axis_index("tp") * seq_part * PHASES + seq_part

    def out_copy(b):
        return pltpu.make_async_copy(rb.at[b], res_ref.at[seq_part + b], rsem.at[seq_part + b])

    def out_copy_a(b):
        return pltpu.make_async_copy(ra_ref.at[:, b * 8:(b + 1) * 8], res_ref.at[b], rsem.at[b])

    def strip(n):
        at = seq_part * rows_tile + n * lane_blocks * 8
        return slice(at, at + lane_blocks * 8)

    def bonus_copy_a(n):
        return pltpu.make_async_copy(ra_ref.at[:, strip(n)], bon_ref.at[n], bsem.at[n])

    width = blocks // (seq_part // group)

    def bonus_copy(g):
        at = pl.ds(g * width, width)
        return pltpu.make_async_copy(bonb.at[:, at], bon_ref.at[strips:, at], bsem.at[strips + g])

    for b in range(seq_part):
        out_copy_a(b).start()
    for n in range(strips):
        bonus_copy_a(n).start()

    for ref, value in zip((mrow, irow, mcol, icol), row_stats(draft, [st_ref[1, n] for n in range(st_ref.shape[1])], seq_part)):
        ref[...] = value
    lane_b = lax.broadcasted_iota(jnp.int32, acc_ref.shape, 1)
    acc_ref[...] = acca_ref[:, :acc_ref.shape[1]]

    @pl.loop(0, seq_part // group)
    def _(g):
        seqs = [g * group + n for n in range(group)]
        m8 = [lane_column(mrow[...], b) for b in seqs]
        i8 = [lane_column(irow[...], b) for b in seqs]
        at_rows = [pl.ds(pl.multiple_of(b * 8, 8), 8) for b in seqs]
        picked = acc_ref[...]
        for n, b in enumerate(seqs):
            ratio = accept_ratio(draft, [x_ref[i, first + b] for i in range(draft)],
                                 lambda pair, row: zb_ref[pair, pl.ds(b * 8 + row, 1), :],
                                 lambda pair, row: q_ref[b, pair, pl.ds(row, 1), :], m8[n], i8[n])
            picked = jnp.where(lane_b == seq_part + b, ratio, picked)
        acc_ref[...] = picked

        def sweep(k, totals):
            totals = list(totals)
            for n, b in enumerate(seqs):
                for j in range(8):
                    at = k * 8 + j
                    excess = jnp.maximum(jnp.exp(zb_ref[at, at_rows[n], :] - m8[n]) * i8[n] - q_ref[b, at], 0.0)
                    rb[b, at] = excess
                    totals[n] += excess
            return tuple(totals)

        totals = lax.fori_loop(0, blocks // 8, sweep, tuple(jnp.zeros((8, LANES), jnp.float32) for _ in seqs))
        inv = [inverse_total(draft, total) for total in totals]

        def scale(k, carry):
            for n, b in enumerate(seqs):
                for j in range(8):
                    rb[b, k * 8 + j] = rb[b, k * 8 + j] * inv[n]
            return carry

        lax.fori_loop(0, blocks // 8, scale, 0)
        for b in seqs:
            out_copy(b).start()

        def bonus(k, carry):
            at = g * width + k
            for n in range(strips):
                for cc in range(lane_blocks):
                    row = strip(n).start + cc * 8
                    seqs8 = slice(n * 8, (n + 1) * 8)
                    bonb[n, at, cc * 8:(cc + 1) * 8, :] = jnp.exp(zb_ref[at, row:row + 8, :] - mcol[seqs8]) * icol[seqs8]
            return carry

        lax.fori_loop(0, width, bonus, 0, unroll=4)
        bonus_copy(g).start()

    run = acc_ref[0:1, :]
    total = run
    for i in range(1, draft):
        run = run * acc_ref[i:i + 1, :]
        total += run
    exp_ref[...] = total

    for n in range(strips):
        bonus_copy_a(n).wait()
    for b in range(seq_part):
        out_copy_a(b).wait()
        out_copy(b).wait()
    for g in range(seq_part // group):
        bonus_copy(g).wait()


def solution(mesh):
    n_dev = mesh.shape["tp"]

    def local_step(hidden, w_shard, q_rows, x_group):
        seqs, npos, depth = hidden.shape
        seq_dev, draft, vocab = q_rows.shape
        shard = w_shard.shape[1]
        blocks = vocab // LANES
        seq_part = seq_dev // PHASES
        seq_unit = PEERS * seq_part
        f32 = jnp.float32
        dma = pltpu.SemaphoreType.DMA
        rows_tile = TILE // LANES * draft
        ksteps = depth // DEPTH
        rows_block = seq_part * (rows_tile + TILE // LANES)
        any_spec = pl.BlockSpec(memory_space=pl.ANY)
        vmem_spec = pl.BlockSpec(memory_space=pltpu.VMEM)
        smem_spec = pl.BlockSpec(memory_space=pltpu.SMEM)
        tokens = x_group.T
        q4 = q_rows.reshape(seq_dev, draft, blocks, LANES).transpose(0, 2, 1, 3).reshape(seq_dev, vocab // TILE, rows_tile, LANES)
        stat_scratch = [pltpu.VMEM((8, LANES), f32)] * 2 + [pltpu.VMEM((seq_part, LANES), f32)] * 2
        res_a, z_b, q_b, st, acc_a = pl.pallas_call(
            functools.partial(exchange_kernel, draft, n_dev),
            out_shape=[pltpu.VMEM((vocab // TILE, rows_block, LANES), f32)] * 2 + [pltpu.VMEM((seq_part, vocab // TILE, rows_tile, LANES), f32)]
                      + [pltpu.VMEM((PHASES, n_dev, 8, LANES), f32), pltpu.VMEM((draft, LANES), f32)],
            in_specs=[any_spec] * 3 + [smem_spec],
            out_specs=[vmem_spec] * 5,
            scratch_shapes=[
                pltpu.VMEM((UNITS, npos, seq_unit, depth), hidden.dtype),
                pltpu.VMEM((2, depth, TILE), w_shard.dtype),
                pltpu.VMEM((npos, seq_unit, TILE), f32),
                pltpu.VMEM((SLOTS, UNITS, PEERS, rows_block, LANES), f32),
                pltpu.VMEM((UNITS, npos, seq_unit, LANES), f32),
                pltpu.VMEM((UNITS, npos, seq_unit, LANES), f32),
                pltpu.VMEM((PHASES, UNITS, PEERS, 8, LANES), f32),
                pltpu.VMEM((vocab // TILE, rows_tile, LANES), f32),
                pltpu.VMEM((vocab // TILE, rows_tile, LANES), f32),
                *stat_scratch,
                dma((UNITS, PEERS, ksteps)), dma((2, ksteps)), dma((2,)), dma((seq_part,)),
                dma((SLOTS, UNITS, PEERS)), dma((PHASES, UNITS, PEERS)), dma((SLOTS,)), dma((PHASES,)),
                dma((PHASES, n_dev)), dma((PHASES, n_dev)),
            ],
            compiler_params=pltpu.CompilerParams(collective_id=0, has_side_effects=True, vmem_limit_bytes=VMEM_LIMIT),
            cost_estimate=pl.CostEstimate(flops=2 * seqs * npos * depth * shard, bytes_accessed=2 * depth * shard, transcendentals=0),
            name="head_exchange",
        )(hidden.transpose(1, 0, 2), w_shard, q4, tokens)

        st, acc_a, res_a, z_b, q_b = (pltpu.with_memory_space_constraint(v, pltpu.VMEM) for v in (st, acc_a, res_a, z_b, q_b))
        accept, expected, res, bonus = pl.pallas_call(
            functools.partial(finish_kernel, draft),
            out_shape=[jax.ShapeDtypeStruct((draft, seq_dev), f32), jax.ShapeDtypeStruct((1, seq_dev), f32),
                       jax.ShapeDtypeStruct((seq_dev, vocab // TILE, rows_tile, LANES), f32),
                       jax.ShapeDtypeStruct((seq_dev // 8, vocab // TILE, TILE // LANES * 8, LANES), f32)],
            in_specs=[smem_spec] + [vmem_spec] * 5,
            out_specs=[vmem_spec] * 2 + [any_spec] * 2,
            scratch_shapes=[
                pltpu.VMEM((seq_part, vocab // TILE, rows_tile, LANES), f32), pltpu.VMEM((seq_part // 8, vocab // TILE, TILE // LANES * 8, LANES), f32), *stat_scratch,
                dma((seq_dev,)), dma((seq_part // 8 + seq_part // 4,)),
            ],
            compiler_params=pltpu.CompilerParams(vmem_limit_bytes=VMEM_LIMIT),
            cost_estimate=pl.CostEstimate(flops=seq_dev * npos * vocab * 8, bytes_accessed=14 * seq_dev * vocab * 4, transcendentals=seq_dev * npos * vocab),
            name="finish_rows",
        )(tokens, st, acc_a, res_a, z_b, q_b)
        residual = res.reshape(seq_dev, blocks, draft, LANES).transpose(0, 2, 1, 3).reshape(seq_dev, draft, vocab)
        return accept.T, expected.reshape(seq_dev), residual, bonus.reshape(seq_dev // 8, vocab // TILE, TILE // LANES, 8, LANES).transpose(0, 3, 1, 2, 4).reshape(seq_dev, vocab)

    return jax.shard_map(local_step, mesh=mesh,
                         in_specs=(P("dp", None, None), P(None, "tp"), P(("dp", "tp"), None, None), P("dp", None)),
                         out_specs=(P(("dp", "tp"), None), P(("dp", "tp")), P(("dp", "tp"), None, None), P(("dp", "tp"), None)),
                         check_vma=False)
```

```python
import functools

import jax
import jax.numpy as jnp
from jax import lax
from jax.experimental import pallas as pl
from jax.experimental.pallas import tpu as pltpu
from jax.sharding import PartitionSpec as P

INV_TEMP = 1.25
LANES = 128
TILE = 256
DEPTH = 3072
SLOTS = 6
CORES = 2
PHASES = 2
UNITS = 2
VMEM_LIMIT = 35 * 1024 * 1024
PEERS = 4


def row_stats(draft, st, seqs):
    m = functools.reduce(jnp.maximum, st)
    inv = 1.0 / sum(pltpu.roll(part, LANES - seqs, 1) * jnp.exp(part - m) for part in st)
    rows = [jnp.concatenate([v[:draft], v[:draft]], axis=0) for v in (m, inv)]
    pad = jnp.zeros((LANES - 8, LANES), jnp.float32)
    cols = [jnp.broadcast_to(jnp.concatenate([v, pad], axis=0).T[:seqs, draft:draft + 1], (seqs, LANES)) for v in (m, inv)]
    return rows + cols


def lane_column(rows, lane):
    hit = lax.broadcasted_iota(jnp.int32, (8, LANES), 1) == lane
    return jnp.broadcast_to(jnp.sum(jnp.where(hit, rows, 0.0), axis=1, keepdims=True), (8, LANES))


def inverse_total(draft, total):
    total += pltpu.roll(total, draft, 0)
    return jnp.broadcast_to(1.0 / jnp.sum(total, axis=1, keepdims=True), (8, LANES))


def accept_ratio(draft, tokens, z_row, q_row, m8, i8):
    lane = lax.broadcasted_iota(jnp.int32, (1, LANES), 1)
    zs, qs = [], []
    for i, x in enumerate(tokens):
        pair, half = lax.shift_right_logical(x, 8), lax.shift_right_logical(x, 7) & 1
        hit = lane == (x & (LANES - 1))
        zs.append(jnp.where(hit, z_row(pair, half * draft + i), 0.0))
        qs.append(jnp.where(hit, q_row(pair, half * draft + i), 0.0))
    z = jnp.sum(jnp.concatenate(zs, axis=0), axis=1, keepdims=True)
    q = jnp.sum(jnp.concatenate(qs, axis=0), axis=1, keepdims=True)
    return jnp.minimum(1.0, jnp.exp(z - m8[:draft, :1]) * i8[:draft, :1] / q)


def exchange_kernel(draft, n_dev, h_ref, w_ref, q_ref, x_ref, za_ref, zb_ref, qb_ref, st_ref, acc_ref,
                    hbuf, wbuf, acc, stage, mrun, srun, stst, qeven, qodd, x_smem, mrow, irow, mcol, icol,
                    xsem, hsem, wsem, qsem, qbsem, ssd, sss, lsd, lss, rsd, rss):
    npos = draft + 1
    chips = n_dev // CORES
    seq_dev = h_ref.shape[1] // n_dev
    seq_part = seq_dev // PHASES
    seq_unit = PEERS * seq_part
    depth = h_ref.shape[2]
    depth_steps = depth // DEPTH
    tiles = w_ref.shape[1] // TILE
    lane_blocks = TILE // LANES
    rows_tile = lane_blocks * draft
    me = lax.axis_index("tp")
    chip, core = me // CORES, lax.rem(me, CORES)

    def is_own(u, n):
        return (2 - u + 2 * (n // CORES)) % chips == 0

    def peer(u, n):
        if is_own(u, n):
            return me if n % CORES else me + 1 - 2 * core
        return lax.rem(chip + 2 - u + 2 * (n // CORES), chips) * CORES + n % CORES

    def h_copies(u, p, k, peers):
        cols = pl.ds(pl.multiple_of(k * DEPTH, DEPTH), DEPTH)
        out = []
        for n in peers:
            rows = pl.ds(pl.multiple_of(peer(u, n) * seq_dev + p * seq_part, seq_part), seq_part)
            out.append(pltpu.make_async_copy(h_ref.at[:, rows, cols], hbuf.at[u, :, n * seq_part:(n + 1) * seq_part, cols], hsem.at[u, n, k]))
        return out

    def w_copy(t, k):
        slot = lax.rem(t, 2)
        rows = pl.ds(pl.multiple_of(k * DEPTH, DEPTH), DEPTH)
        col = pl.multiple_of(lax.rem(t, tiles) * TILE, TILE)
        return pltpu.make_async_copy(w_ref.at[rows, pl.ds(col, TILE)], wbuf.at[slot, rows], wsem.at[slot, k])

    def pieces(t, u, p, peers):
        slot = lax.rem(t, SLOTS)
        block = me * tiles + lax.rem(t, tiles)
        out = []
        for n in peers:
            src, dst = stage.at[slot, u, n], (za_ref, zb_ref)[p].at[block]
            if is_own(u, n) and n % CORES:
                out.append(pltpu.make_async_copy(src, dst, lsd.at[slot]))
            else:
                out.append(pltpu.make_async_remote_copy(src, dst, ssd.at[slot, u, n], rsd.at[p, me], device_id={"tp": peer(u, n)}))
        return out

    def stat_pieces(p, u):
        out = []
        for n in range(PEERS):
            src, dst = stst.at[p, u, n], st_ref.at[p, me]
            if is_own(u, n) and n % CORES:
                out.append(pltpu.make_async_copy(src, dst, lss.at[p]))
            else:
                out.append(pltpu.make_async_remote_copy(src, dst, sss.at[p, u, n], rss.at[p, me], device_id={"tp": peer(u, n)}))
        return out

    def wait_sent(copies):
        for copy in copies:
            copy.wait_send() if copy.is_remote else copy.wait()

    def wait_received(p):
        for o in range(1, n_dev):
            src = lax.rem(me + o, n_dev)
            zrows = (za_ref, zb_ref)[p].at[pl.ds(src * tiles, tiles)]
            pltpu.make_async_copy(zrows, zrows, rsd.at[p, src]).wait()
            pltpu.make_async_copy(st_ref.at[p, src], st_ref.at[p, src], rss.at[p, src]).wait()

    finish_from = tiles + SLOTS + 1

    def q_copy(n, u):
        return pltpu.make_async_copy(q_ref.at[2 * n + u], (qeven, qodd)[u], qsem.at[u])

    def qb_copy(b):
        return pltpu.make_async_copy(q_ref.at[seq_part + b], qb_ref.at[b], qbsem.at[b])

    def finish(b, q_buf):
        m8, i8 = lane_column(mrow[...], b), lane_column(irow[...], b)
        rows = pl.multiple_of(b * 8, 8)
        first = me * seq_dev + b
        ratio = accept_ratio(draft, [x_smem[i, first] for i in range(draft)],
                             lambda pair, row: za_ref[pair, pl.ds(rows + row, 1), :],
                             lambda pair, row: q_buf[pair, pl.ds(row, 1), :], m8, i8)
        lane = lax.broadcasted_iota(jnp.int32, acc_ref.shape, 1)
        acc_ref[...] = jnp.where(lane == b, ratio, acc_ref[...])
        group = 16
        blocks = za_ref.shape[0]

        def sweep(n, totals):
            totals = list(totals)
            for g in range(group):
                at = n * group + g
                excess = jnp.maximum(jnp.exp(za_ref[at, pl.ds(rows, 8), :] - m8) * i8 - q_buf[at], 0.0)
                za_ref[at, pl.ds(rows, 8), :] = excess
                totals[g % 4] += excess
            return tuple(totals)

        totals = lax.fori_loop(0, blocks // group, sweep, tuple(jnp.zeros((8, LANES), jnp.float32) for _ in range(4)))
        inv = inverse_total(draft, sum(totals))

        def scale(n, carry):
            for g in range(group):
                at = n * group + g
                za_ref[at, pl.ds(rows, 8), :] = za_ref[at, pl.ds(rows, 8), :] * inv
            return carry

        lax.fori_loop(0, blocks // group, scale, 0)
        part = blocks // seq_part
        for n in range(part):
            for row in range(0, seq_part, 8):
                for cc in range(lane_blocks):
                    at = pl.ds(seq_part * rows_tile + row * lane_blocks + cc * 8, 8)
                    za_ref[b * part + n, at, :] = jnp.exp(za_ref[b * part + n, at, :] - mcol[row:row + 8]) * icol[row:row + 8]

    everyone, far, own = tuple(range(PEERS)), tuple(range(CORES)), tuple(range(CORES, PEERS))
    last = PHASES * tiles - 1

    def start_all(copies):
        for copy in copies:
            copy.start()

    for k in range(depth_steps):
        start_all(h_copies(0, 0, k, far))
        w_copy(0, k).start()
    x_copy = pltpu.make_async_copy(x_ref, x_smem, xsem)
    x_copy.start()

    barrier = pltpu.get_barrier_semaphore()
    for o in range(1, n_dev):
        pl.semaphore_signal(barrier, 1, device_id={"tp": lax.rem(me + o, n_dev)})
    pl.semaphore_wait(barrier, n_dev - 1)

    def multiply_as_it_comes(t, u, peers):
        p = t // tiles
        rows = slice(peers[0] * seq_part, (peers[-1] + 1) * seq_part)
        count = len(peers) * seq_part
        acc[:, rows, :] = jnp.zeros((npos, count, TILE), jnp.float32)
        mrun[u] = jnp.full(mrun.shape[1:], -jnp.inf, jnp.float32)
        srun[u] = jnp.zeros(srun.shape[1:], jnp.float32)

        @pl.loop(0, depth_steps)
        def _(k):
            for copy in h_copies(u, p, k, peers):
                copy.wait()
            if peers == far:
                w_copy(t, k).wait()
                start_all(h_copies(1, p, k, everyone))
            else:
                start_all(h_copies(0, p, k, own))
                w_copy(t + 1, k).start()
            cols = pl.ds(pl.multiple_of(k * DEPTH, DEPTH), DEPTH)
            lhs = hbuf[u, :, rows, cols].reshape(npos * count, DEPTH)
            prod = jnp.dot(lhs, wbuf[lax.rem(t, 2), cols, :], preferred_element_type=jnp.float32)
            acc[:, rows, :] += prod.reshape(npos, count, TILE)

    def multiply(t, u):
        if u == 0:
            for k in range(depth_steps):
                w_copy(t, k).wait()
        else:
            @pl.when(t < last)
            def _():
                for k in range(depth_steps):
                    w_copy(t + 1, k).start()
        prod = jnp.dot(hbuf[u].reshape(npos * seq_unit, depth), wbuf[lax.rem(t, 2)], preferred_element_type=jnp.float32)
        acc[...] = prod.reshape(acc.shape)

    def multiply_own(t):
        rows = slice(CORES * seq_part, seq_unit)
        count = seq_unit - CORES * seq_part
        prod = jnp.dot(hbuf[0, :, rows].reshape(npos * count, depth), wbuf[lax.rem(t, 2)], preferred_element_type=jnp.float32)
        acc[:, rows, :] = prod.reshape(npos, count, TILE)

    def send(t, u, peers):
        slot, p = lax.rem(t, SLOTS), t // tiles

        @pl.when(t >= SLOTS)
        def _():
            wait_sent(pieces(t - SLOTS, u, 0, peers))

        rows = slice(peers[0] * seq_part, (peers[-1] + 1) * seq_part)
        for i in range(npos):
            zs = [acc[i, rows, cc * LANES:(cc + 1) * LANES] * INV_TEMP for cc in range(lane_blocks)]
            m_old = mrun[u, i, rows]
            m_new = functools.reduce(jnp.maximum, zs, m_old)
            total = srun[u, i, rows] * jnp.exp(m_old - m_new)
            for cc, z in enumerate(zs):
                total += jnp.exp(z - m_new)
                for at_n, n in enumerate(peers):
                    z_n = z[at_n * seq_part:(at_n + 1) * seq_part]
                    if i < draft:
                        stage[slot, u, n, pl.ds(cc * draft + i, seq_part, stride=rows_tile), :] = z_n
                    else:
                        for row in range(0, seq_part, 8):
                            at = seq_part * rows_tile + row * lane_blocks + cc * 8
                            stage[slot, u, n, at:at + 8, :] = z_n[row:row + 8]
            mrun[u, i, rows] = m_new
            srun[u, i, rows] = total
        for static_p in range(PHASES):
            @pl.when(p == static_p)
            def _():
                start_all(pieces(t, u, static_p, peers))

    @pl.loop(0, PHASES * tiles)
    def _(t):
        p, j = t // tiles, lax.rem(t, tiles)
        for u in range(UNITS):
            peers = far if u == 0 else everyone

            @pl.when(j == 0)
            def _():
                multiply_as_it_comes(t, u, peers)

            if u == 0:
                @pl.when(j == 1)
                def _():
                    for k in range(depth_steps):
                        for copy in h_copies(0, p, k, own):
                            copy.wait()

            @pl.when(j > 0)
            def _():
                multiply(t, u)

            if u == 0:
                @pl.when((j == tiles - 1) & (p + 1 < PHASES))
                def _():
                    for k in range(depth_steps):
                        start_all(h_copies(0, p + 1, k, far))

            send(t, u, peers)
            if u == 0:
                @pl.when(j > 0)
                def _():
                    send(t, 0, own)

                @pl.when(j == 1)
                def _():
                    multiply_own(t - 1)
                    send(t - 1, 0, own)

            @pl.when(j == tiles - 1)
            def _():
                lane = lax.broadcasted_iota(jnp.int32, (seq_unit, LANES), 1)
                packed = jnp.zeros((seq_unit, LANES), jnp.float32)
                for i in range(npos):
                    m_lane = mrun[u, i]
                    m = jnp.max(m_lane, axis=1, keepdims=True)
                    s = jnp.sum(srun[u, i] * jnp.exp(m_lane - m), axis=1, keepdims=True)
                    packed = jnp.where(lane == i, m, packed)
                    packed = jnp.where(lane == 8 + i, s, packed)
                flat = jnp.concatenate([packed, jnp.zeros((LANES - seq_unit, LANES), jnp.float32)], axis=0).T[:16]
                for n in range(PEERS):
                    m_n, s_n = (pltpu.roll(v, (LANES - n * seq_part + shift) % LANES, 1) for v, shift in ((flat[:8], 0), (flat[8:], seq_part)))
                    stst[p, u, n] = jnp.where(lane[:8] < seq_part, m_n, s_n)
                for copy in stat_pieces(p, u):
                    copy.start()

            if u == 0:
                @pl.when((t >= tiles) & (t < tiles + seq_part))
                def _():
                    qb_copy(t - tiles).start()

            @pl.when(t == finish_from - 1)
            def _():
                q_copy(0, u).start()

            @pl.when((t >= finish_from) & (t < finish_from + seq_part // 2))
            def _():
                if u == 0:
                    @pl.when(t == finish_from)
                    def _():
                        for unit in range(UNITS):
                            wait_sent(stat_pieces(0, unit))
                        wait_received(0)
                        x_copy.wait()
                        for ref, value in zip((mrow, irow, mcol, icol), row_stats(draft, [st_ref[0, n] for n in range(n_dev)], seq_part)):
                            ref[...] = value
                        acc_ref[...] = jnp.zeros(acc_ref.shape, jnp.float32)
                q_copy(t - finish_from, u).wait()
                finish(2 * (t - finish_from) + u, (qeven, qodd)[u])

                @pl.when(t + 1 < finish_from + seq_part // 2)
                def _():
                    q_copy(t + 1 - finish_from, u).start()

    for t in range(PHASES * tiles - SLOTS, PHASES * tiles):
        for u in range(UNITS):
            wait_sent(pieces(t, u, 1, everyone))
    for u in range(UNITS):
        wait_sent(stat_pieces(1, u))
    for b in range(seq_part):
        qb_copy(b).wait()
    wait_received(1)


def finish_kernel(draft, x_ref, st_ref, acca_ref, ra_ref, zb_ref, q_ref, acc_out, exp_out, res_ref, bon_ref,
                  rb, bonb, acc_ref, exp_ref, x_smem, mrow, irow, mcol, icol, rsem, bsem, xsem, asem):
    blocks = zb_ref.shape[0]
    seq_part, _, rows_tile, _ = q_ref.shape
    lane_blocks = rows_tile // draft
    strips = seq_part // 8
    group = 4
    first = lax.axis_index("tp") * seq_part * PHASES + seq_part

    def out_copy(b):
        return pltpu.make_async_copy(rb.at[b], res_ref.at[seq_part + b], rsem.at[seq_part + b])

    def out_copy_a(b):
        return pltpu.make_async_copy(ra_ref.at[:, b * 8:(b + 1) * 8], res_ref.at[b], rsem.at[b])

    def strip(n):
        at = seq_part * rows_tile + n * lane_blocks * 8
        return slice(at, at + lane_blocks * 8)

    def bonus_copy_a(n):
        return pltpu.make_async_copy(ra_ref.at[:, strip(n)], bon_ref.at[n], bsem.at[n])

    width = blocks // (seq_part // group)

    def bonus_copy(g):
        at = pl.ds(g * width, width)
        return pltpu.make_async_copy(bonb.at[:, at], bon_ref.at[strips:, at], bsem.at[strips + g])

    x_copy = pltpu.make_async_copy(x_ref, x_smem, xsem)
    x_copy.start()
    for b in range(seq_part):
        out_copy_a(b).start()
    for n in range(strips):
        bonus_copy_a(n).start()

    for ref, value in zip((mrow, irow, mcol, icol), row_stats(draft, [st_ref[1, n] for n in range(st_ref.shape[1])], seq_part)):
        ref[...] = value
    lane_b = lax.broadcasted_iota(jnp.int32, acc_ref.shape, 1)
    acc_ref[...] = acca_ref[:, :acc_ref.shape[1]]
    x_copy.wait()

    @pl.loop(0, seq_part // group)
    def _(g):
        seqs = [g * group + n for n in range(group)]
        m8 = [lane_column(mrow[...], b) for b in seqs]
        i8 = [lane_column(irow[...], b) for b in seqs]
        at_rows = [pl.ds(pl.multiple_of(b * 8, 8), 8) for b in seqs]
        picked = acc_ref[...]
        for n, b in enumerate(seqs):
            ratio = accept_ratio(draft, [x_smem[i, first + b] for i in range(draft)],
                                 lambda pair, row: zb_ref[pair, pl.ds(b * 8 + row, 1), :],
                                 lambda pair, row: q_ref[b, pair, pl.ds(row, 1), :], m8[n], i8[n])
            picked = jnp.where(lane_b == seq_part + b, ratio, picked)
        acc_ref[...] = picked

        def sweep(k, totals):
            totals = list(totals)
            for n, b in enumerate(seqs):
                for j in range(8):
                    at = k * 8 + j
                    excess = jnp.maximum(jnp.exp(zb_ref[at, at_rows[n], :] - m8[n]) * i8[n] - q_ref[b, at], 0.0)
                    rb[b, at] = excess
                    totals[n] += excess
            return tuple(totals)

        totals = lax.fori_loop(0, blocks // 8, sweep, tuple(jnp.zeros((8, LANES), jnp.float32) for _ in seqs))
        inv = [inverse_total(draft, total) for total in totals]

        def scale(k, carry):
            for n, b in enumerate(seqs):
                for j in range(8):
                    rb[b, k * 8 + j] = rb[b, k * 8 + j] * inv[n]
            return carry

        lax.fori_loop(0, blocks // 8, scale, 0)
        for b in seqs:
            out_copy(b).start()

        def bonus(k, carry):
            at = g * width + k
            for n in range(strips):
                for cc in range(lane_blocks):
                    row = strip(n).start + cc * 8
                    seqs8 = slice(n * 8, (n + 1) * 8)
                    bonb[n, at, cc * 8:(cc + 1) * 8, :] = jnp.exp(zb_ref[at, row:row + 8, :] - mcol[seqs8]) * icol[seqs8]
            return carry

        lax.fori_loop(0, width, bonus, 0, unroll=4)
        bonus_copy(g).start()

    run = acc_ref[0:1, :]
    total = run
    for i in range(1, draft):
        run = run * acc_ref[i:i + 1, :]
        total += run
    exp_ref[...] = total
    small = [pltpu.make_async_copy(src, dst, asem.at[n]) for n, (src, dst) in enumerate(((acc_ref, acc_out), (exp_ref, exp_out)))]
    for copy in small:
        copy.start()

    for copy in small:
        copy.wait()
    for n in range(strips):
        bonus_copy_a(n).wait()
    for b in range(seq_part):
        out_copy_a(b).wait()
        out_copy(b).wait()
    for g in range(seq_part // group):
        bonus_copy(g).wait()


def solution(mesh):
    n_dev = mesh.shape["tp"]

    def local_step(hidden, w_shard, q_rows, x_group):
        seqs, npos, depth = hidden.shape
        seq_dev, draft, vocab = q_rows.shape
        shard = w_shard.shape[1]
        blocks = vocab // LANES
        seq_part = seq_dev // PHASES
        seq_unit = PEERS * seq_part
        f32 = jnp.float32
        dma = pltpu.SemaphoreType.DMA
        rows_tile = TILE // LANES * draft
        ksteps = depth // DEPTH
        rows_block = seq_part * (rows_tile + TILE // LANES)
        any_spec = pl.BlockSpec(memory_space=pl.ANY)
        vmem_spec = pl.BlockSpec(memory_space=pltpu.VMEM)
        tokens = x_group.T
        q4 = q_rows.reshape(seq_dev, draft, blocks, LANES).transpose(0, 2, 1, 3).reshape(seq_dev, vocab // TILE, rows_tile, LANES)
        stat_scratch = [pltpu.VMEM((8, LANES), f32)] * 2 + [pltpu.VMEM((seq_part, LANES), f32)] * 2
        res_a, z_b, q_b, st, acc_a = pl.pallas_call(
            functools.partial(exchange_kernel, draft, n_dev),
            out_shape=[pltpu.VMEM((vocab // TILE, rows_block, LANES), f32)] * 2 + [pltpu.VMEM((seq_part, vocab // TILE, rows_tile, LANES), f32)]
                      + [pltpu.VMEM((PHASES, n_dev, 8, LANES), f32), pltpu.VMEM((draft, LANES), f32)],
            in_specs=[any_spec] * 4,
            out_specs=[vmem_spec] * 5,
            scratch_shapes=[
                pltpu.VMEM((UNITS, npos, seq_unit, depth), hidden.dtype),
                pltpu.VMEM((2, depth, TILE), w_shard.dtype),
                pltpu.VMEM((npos, seq_unit, TILE), f32),
                pltpu.VMEM((SLOTS, UNITS, PEERS, rows_block, LANES), f32),
                pltpu.VMEM((UNITS, npos, seq_unit, LANES), f32),
                pltpu.VMEM((UNITS, npos, seq_unit, LANES), f32),
                pltpu.VMEM((PHASES, UNITS, PEERS, 8, LANES), f32),
                pltpu.VMEM((vocab // TILE, rows_tile, LANES), f32),
                pltpu.VMEM((vocab // TILE, rows_tile, LANES), f32),
                pltpu.SMEM((draft, seqs), jnp.int32), *stat_scratch,
                dma, dma((UNITS, PEERS, ksteps)), dma((2, ksteps)), dma((2,)), dma((seq_part,)),
                dma((SLOTS, UNITS, PEERS)), dma((PHASES, UNITS, PEERS)), dma((SLOTS,)), dma((PHASES,)),
                dma((PHASES, n_dev)), dma((PHASES, n_dev)),
            ],
            compiler_params=pltpu.CompilerParams(collective_id=0, has_side_effects=True, vmem_limit_bytes=VMEM_LIMIT),
            cost_estimate=pl.CostEstimate(flops=2 * seqs * npos * depth * shard, bytes_accessed=2 * depth * shard, transcendentals=0),
            name="head_exchange",
        )(hidden.transpose(1, 0, 2), w_shard, q4, tokens)

        st, acc_a, res_a, z_b, q_b = (pltpu.with_memory_space_constraint(v, pltpu.VMEM) for v in (st, acc_a, res_a, z_b, q_b))
        accept, expected, res, bonus = pl.pallas_call(
            functools.partial(finish_kernel, draft),
            out_shape=[jax.ShapeDtypeStruct((draft, seq_dev), f32), jax.ShapeDtypeStruct((1, seq_dev), f32),
                       jax.ShapeDtypeStruct((seq_dev, vocab // TILE, rows_tile, LANES), f32),
                       jax.ShapeDtypeStruct((seq_dev // 8, vocab // TILE, TILE // LANES * 8, LANES), f32)],
            in_specs=[any_spec] + [vmem_spec] * 5,
            out_specs=[any_spec] * 4,
            scratch_shapes=[
                pltpu.VMEM((seq_part, vocab // TILE, rows_tile, LANES), f32), pltpu.VMEM((seq_part // 8, vocab // TILE, TILE // LANES * 8, LANES), f32),
                pltpu.VMEM((draft, seq_dev), f32), pltpu.VMEM((1, seq_dev), f32), pltpu.SMEM((draft, seqs), jnp.int32), *stat_scratch,
                dma((seq_dev,)), dma((seq_part // 8 + seq_part // 4,)), dma, dma((2,)),
            ],
            compiler_params=pltpu.CompilerParams(vmem_limit_bytes=VMEM_LIMIT),
            cost_estimate=pl.CostEstimate(flops=seq_dev * npos * vocab * 8, bytes_accessed=14 * seq_dev * vocab * 4, transcendentals=seq_dev * npos * vocab),
            name="finish_rows",
        )(tokens, st, acc_a, res_a, z_b, q_b)
        residual = res.reshape(seq_dev, blocks, draft, LANES).transpose(0, 2, 1, 3).reshape(seq_dev, draft, vocab)
        return accept.T, expected.reshape(seq_dev), residual, bonus.reshape(seq_dev // 8, vocab // TILE, TILE // LANES, 8, LANES).transpose(0, 3, 1, 2, 4).reshape(seq_dev, vocab)

    return jax.shard_map(local_step, mesh=mesh,
                         in_specs=(P("dp", None, None), P(None, "tp"), P(("dp", "tp"), None, None), P("dp", None)),
                         out_specs=(P(("dp", "tp"), None), P(("dp", "tp")), P(("dp", "tp"), None, None), P(("dp", "tp"), None)),
                         check_vma=False)
```
